16 devices in a mesh: ez: 2 (over z), ey: 2 (over y), ex: 4 (over x, core).
Axes of the slice: x: 2, y: 2, z: 2, core: 2. Of those that a mesh axis runs over, the one named last changes fastest.
Arguments:
- tokens: bfloat16 [4096, 2048], P(('ez', 'ey', 'ex'))
- expert_ids: int32 [4096, 8], P(('ez', 'ey', 'ex'))
- gate_weights: float32 [4096, 8], P(('ez', 'ey', 'ex'))
- w_gate: bfloat16 [64, 2048, 1024], P(('ez', 'ey', 'ex'))
- w_up: bfloat16 [64, 2048, 1024], P(('ez', 'ey', 'ex'))
- w_down: bfloat16 [64, 1024, 2048], P(('ez', 'ey', 'ex'))
Outputs:
- output: bfloat16 [4096, 2048], P(('ez', 'ey', 'ex'))
All inputs are finite; a program needn't handle non-finite values.
Results may differ from the reference program's by a relative error of at most 0.00588.
Values are sent between devices in bfloat16 or wider.
A program may use at most 1 GiB of HBM per device.

```python
import jax
import jax.numpy as jnp
from jax import lax

HIDDEN = 2048
EXPERT_FF = 1024
EXPERTS = 64
TOP_K = 8
TOKENS = 256
DEVICES = 16
TOTAL_TOK = DEVICES * TOKENS
LOCAL_EXPERTS = EXPERTS // DEVICES
PER_EXPERT = TOTAL_TOK * TOP_K // EXPERTS


def draw_routing(route_key):
    def one_source(src_key):
        key_first, key_rest, key_dev, key_order = jax.random.split(src_key, 4)
        first_block = jax.random.permutation(key_first, LOCAL_EXPERTS)
        rest_block = jax.random.permutation(key_rest, EXPERTS - LOCAL_EXPERTS) + LOCAL_EXPERTS
        positions = jnp.arange(EXPERTS)
        spaced = positions % DEVICES == 0
        first_idx = jnp.clip(positions // DEVICES, 0, LOCAL_EXPERTS - 1)
        rest_idx = jnp.clip(positions - positions // DEVICES - 1, 0, EXPERTS - LOCAL_EXPERTS - 1)
        expert_cycle = jnp.where(spaced, first_block[first_idx], rest_block[rest_idx])
        dev_perm = jax.random.permutation(key_dev, DEVICES)
        expert_cycle = dev_perm[expert_cycle // LOCAL_EXPERTS] * LOCAL_EXPERTS + expert_cycle % LOCAL_EXPERTS
        tok_perm = jax.random.permutation(key_order, TOKENS)
        slot_pos = tok_perm[:, None] * TOP_K + jnp.arange(TOP_K)[None, :]
        return expert_cycle[slot_pos % EXPERTS]
    src_keys = jax.random.split(route_key, DEVICES)
    return jax.vmap(one_source)(src_keys).reshape(TOTAL_TOK, TOP_K).astype(jnp.int32)


def setup_inputs(seed: int = 0) -> dict:
    root_key = jax.random.key(seed)
    key_tok, key_ids, key_gate, key_w1, key_w3, key_w2 = jax.random.split(root_key, 6)
    tokens = jax.random.normal(key_tok, (TOTAL_TOK, HIDDEN), jnp.float32).astype(jnp.bfloat16)
    expert_ids = draw_routing(key_ids)
    gate_logits = 0.7 * jax.random.normal(key_gate, (TOTAL_TOK, TOP_K), jnp.float32)
    gate_weights = jax.nn.softmax(gate_logits, axis=-1)
    w_gate = (jax.random.normal(key_w1, (EXPERTS, HIDDEN, EXPERT_FF), jnp.float32) * HIDDEN ** -0.5).astype(jnp.bfloat16)
    w_up = (jax.random.normal(key_w3, (EXPERTS, HIDDEN, EXPERT_FF), jnp.float32) * HIDDEN ** -0.5).astype(jnp.bfloat16)
    w_down = (jax.random.normal(key_w2, (EXPERTS, EXPERT_FF, HIDDEN), jnp.float32) * (2.0 * EXPERT_FF ** -0.5)).astype(jnp.bfloat16)
    return {"tokens": tokens, "expert_ids": expert_ids, "gate_weights": gate_weights, "w_gate": w_gate, "w_up": w_up, "w_down": w_down}


def reference(tokens, expert_ids, gate_weights, w_gate, w_up, w_down):
    sort_order = jnp.argsort(expert_ids.reshape(-1), stable=True)
    rows_by_expert = (sort_order // TOP_K).reshape(EXPERTS, PER_EXPERT)
    gates_by_expert = gate_weights.reshape(-1)[sort_order].reshape(EXPERTS, PER_EXPERT)

    def expert_step(acc_out, expert_args):
        row_ids, row_gates, gate_mat, up_mat, down_mat = expert_args
        x_rows = tokens[row_ids]
        gate_act = jnp.dot(x_rows, gate_mat, preferred_element_type=jnp.float32)
        up_act = jnp.dot(x_rows, up_mat, preferred_element_type=jnp.float32)
        hidden_act = (jax.nn.silu(gate_act) * up_act).astype(jnp.bfloat16)
        expert_out = jnp.dot(hidden_act, down_mat, preferred_element_type=jnp.float32)
        acc_out = acc_out.at[row_ids].add(expert_out * row_gates[:, None])
        return acc_out, None

    init_acc = jnp.zeros((TOTAL_TOK, HIDDEN), jnp.float32)
    moe_sum = lax.scan(expert_step, init_acc, (rows_by_expert, gates_by_expert, w_gate, w_up, w_down))[0]
    return (tokens.astype(jnp.float32) + moe_sum).astype(jnp.bfloat16)
```

```python
import math
import jax
import jax.numpy as jnp
from jax import lax
from jax.sharding import PartitionSpec as P


def solution(mesh):
    ep_axes = tuple(mesh.axis_names)
    num_devices = math.prod(mesh.shape[axis_name] for axis_name in ep_axes)
    row_spec = P(ep_axes, None)
    w_spec = P(ep_axes, None, None)

    def local_layer(tokens, expert_ids, gate_weights, w_gate, w_up, w_down):
        tok_dev, hidden = tokens.shape
        top_k = expert_ids.shape[1]
        local_experts = w_gate.shape[0]
        capacity = tok_dev * top_k // num_devices
        rows = num_devices * capacity
        per_expert = rows // local_experts
        x_all = lax.all_gather(tokens, ep_axes, axis=0, tiled=True)
        all_experts = jnp.arange(num_devices * local_experts)
        gate_dense = jnp.sum(jnp.where(expert_ids[:, :, None] == all_experts[None, None, :], gate_weights[:, :, None], 0.0), axis=1)
        gate_send = gate_dense.reshape(tok_dev, num_devices, local_experts).transpose(1, 2, 0)
        gates = lax.all_to_all(gate_send, ep_axes, 0, 0, tiled=True)
        hit = jnp.any(gates > 0.0, axis=1)
        slot = jnp.where(hit, jnp.cumsum(hit.astype(jnp.int32), axis=1) - 1, -1)
        place = slot[:, None, :] == jnp.arange(capacity)[None, :, None]
        place_bf = place.astype(jnp.bfloat16)
        packed = jnp.einsum("sct,sth->sch", place_bf, x_all.reshape(num_devices, tok_dev, hidden), preferred_element_type=jnp.float32).astype(jnp.bfloat16)
        packed = packed.reshape(rows, hidden)
        gate_pack = jnp.sum(jnp.where(place[:, None], gates[:, :, None, :], 0.0), axis=3)
        gate_pack = gate_pack.transpose(1, 0, 2).reshape(local_experts, rows)
        chosen = gate_pack > 0.0
        rank = jnp.where(chosen, jnp.cumsum(chosen.astype(jnp.int32), axis=1) - 1, -1)
        pick = rank[:, None, :] == jnp.arange(per_expert)[None, :, None]
        pick_bf = pick.astype(jnp.bfloat16)
        pick_gates = jnp.sum(jnp.where(pick, gate_pack[:, None, :], 0.0), axis=2)
        x_exp = jnp.einsum("eir,rh->eih", pick_bf, packed, preferred_element_type=jnp.float32).astype(jnp.bfloat16)
        gate_act = jnp.einsum("lch,lhf->lcf", x_exp, w_gate, preferred_element_type=jnp.float32)
        up_act = jnp.einsum("lch,lhf->lcf", x_exp, w_up, preferred_element_type=jnp.float32)
        hidden_act = (jax.nn.silu(gate_act) * up_act).astype(jnp.bfloat16)
        out = jnp.einsum("lcf,lfh->lch", hidden_act, w_down, preferred_element_type=jnp.float32) * pick_gates[:, :, None]
        out_hi = lax.reduce_precision(out, 8, 7)
        out_lo = (out - out_hi).astype(jnp.bfloat16)
        out_hi = out_hi.astype(jnp.bfloat16)
        part = jnp.einsum("eir,eih->rh", pick_bf, out_hi, preferred_element_type=jnp.float32)
        part = part + jnp.einsum("eir,eih->rh", pick_bf, out_lo, preferred_element_type=jnp.float32)
        part = part.astype(jnp.bfloat16).reshape(num_devices, capacity, hidden)
        dense = jnp.einsum("sct,sch->sth", place_bf, part, preferred_element_type=jnp.float32).astype(jnp.bfloat16)
        moe_sum = lax.psum_scatter(dense.reshape(num_devices * tok_dev, hidden), ep_axes, scatter_dimension=0, tiled=True)
        return (tokens.astype(jnp.float32) + moe_sum.astype(jnp.float32)).astype(jnp.bfloat16)

    return jax.shard_map(local_layer, mesh=mesh, in_specs=(row_spec, row_spec, row_spec, w_spec, w_spec, w_spec), out_specs=row_spec, check_vma=False)
```

```python
import math
import jax
import jax.numpy as jnp
from jax import lax
from jax.experimental import pallas as pl
from jax.experimental.pallas import tpu as pltpu
from jax.sharding import PartitionSpec as P

MESH = pl.DeviceIdType.MESH
CW = 256
ROW_PARTS = ((0, 96), (96, 80), (176, 80))
ALL = slice(None)
GATHER_STEPS = (
    (("x", (0, 0, 0), (0, 0, 1)), ("y", (0, 0, ALL), (0, 1, ALL)), ("z", (0, ALL, ALL), (1, ALL, ALL))),
    (("y", (0, 0, 0), (0, 1, 0)), ("z", (0, ALL, 0), (1, ALL, 0)), ("x", (ALL, ALL, 0), (ALL, ALL, 1))),
    (("z", (0, 0, 0), (1, 0, 0)), ("x", (ALL, 0, 0), (ALL, 0, 1)), ("y", (ALL, 0, ALL), (ALL, 1, ALL))),
)
SCATTER_STEPS = tuple(tuple((link, dst, src) for link, src, dst in steps[::-1]) for steps in GATHER_STEPS)
LANDING = ((1, 0, ALL, ALL), (1, 1, 0, ALL), (1, 1, 1, 0))


def moe_kernel(x_hbm, slot_row, slot_col, rank_row, rank_col, gate_row, w1_hbm, w3_hbm, w2_hbm, out_ref,
               g_buf, acc, sel, dense, hid, w13, w2, pair, x_exp, x_res, gate_col,
               step_send, step_recv, core_send, core_recv, x_sem, w13_sem, w2_sem, res_sem, ready):
    zb, yb, ex = lax.axis_index("ez"), lax.axis_index("ey"), lax.axis_index("ex")
    xb, cb = ex // 2, ex % 2
    peers = {
        "x": (zb, yb, (1 - xb) * 2 + cb),
        "y": (zb, 1 - yb, ex),
        "z": (1 - zb, yb, ex),
        "core": (zb, yb, xb * 2 + 1 - cb),
    }
    tok = x_hbm.shape[0]
    hidden = x_hbm.shape[1]
    chunks = hidden // CW
    experts, _, ff = w1_hbm.shape
    sources = slot_row.shape[0]
    rows = rank_col.shape[0]
    cap = rows // sources
    per_expert = rows // experts

    def xor(a, b):
        return a + b - 2 * a * b

    def source_of(rel):
        return (xor(zb, rel // 4 % 2) * 8 + xor(yb, rel // 2 % 2) * 4 + xor(xb, rel % 2) * 2 + xor(cb, rel // 8))

    def gather_copy(c, part, step):
        r0, n = ROW_PARTS[part]
        link, src, dst = GATHER_STEPS[part][step]
        return pltpu.make_async_remote_copy(
            g_buf.at[(c, 0) + src + (pl.ds(r0, n),)], g_buf.at[(c, 0) + dst + (pl.ds(r0, n),)],
            step_send.at[c, part, step], step_recv.at[c, part, step], device_id=peers[link], device_id_type=MESH)

    def gather_core(c):
        return pltpu.make_async_remote_copy(g_buf.at[c, 0], g_buf.at[c, 1], core_send.at[c], core_recv.at[c],
                                            device_id=peers["core"], device_id_type=MESH)

    def scatter_core(k):
        return pltpu.make_async_remote_copy(dense.at[k % 2, 1], g_buf.at[k, 0], core_send.at[k], core_recv.at[k],
                                            device_id=peers["core"], device_id_type=MESH)

    def scatter_copy(k, part, step):
        r0, n = ROW_PARTS[part]
        link, src, _ = SCATTER_STEPS[part][step]
        return pltpu.make_async_remote_copy(
            g_buf.at[(k, 0) + src + (pl.ds(r0, n),)], g_buf.at[(k,) + LANDING[step] + (pl.ds(r0, n),)],
            step_send.at[k, part, step], step_recv.at[k, part, step], device_id=peers[link], device_id_type=MESH)

    def x_copy(c):
        cols = pl.ds(pl.multiple_of(c * CW, CW), CW)
        return pltpu.make_async_copy(x_hbm.at[:, cols], g_buf.at[c, 0, 0, 0, 0], x_sem.at[c])

    def w13_copies(i):
        c, e, b = i // experts, i % experts, i % 2
        k_rows = pl.ds(pl.multiple_of(c * CW, CW), CW)
        return (pltpu.make_async_copy(w1_hbm.at[e, k_rows], w13.at[b, 0], w13_sem.at[b, 0]),
                pltpu.make_async_copy(w3_hbm.at[e, k_rows], w13.at[b, 1], w13_sem.at[b, 1]))

    def w2_copy(i):
        k, e, b = i // experts, i % experts, i % 2
        cols = pl.ds(pl.multiple_of(k * CW, CW), CW)
        return pltpu.make_async_copy(w2_hbm.at[e, :, cols], w2.at[b], w2_sem.at[b])

    def each(parts, fn):
        for part in parts:
            fn(part)

    PARTS = range(len(ROW_PARTS))

    for c in range(chunks):
        x_copy(c).start()
    res_copy = pltpu.make_async_copy(x_hbm, x_res, res_sem)
    res_copy.start()
    for i in range(2):
        for copy in w13_copies(i):
            copy.start()
        w2_copy(i).start()
    barrier = pltpu.get_barrier_semaphore()
    for peer in peers.values():
        pl.semaphore_signal(barrier, inc=1, device_id=peer, device_id_type=MESH)
    pl.semaphore_wait(barrier, len(peers))

    def start_first(c):
        x_copy(c).wait()
        each(PARTS, lambda p: gather_copy(c, p, 0).start())

    def advance(c, step):
        def one(p):
            gather_copy(c, p, step - 1).wait_recv()
            gather_copy(c, p, step).start()
        each(PARTS, one)

    def to_core(c):
        each(PARTS, lambda p: gather_copy(c, p, 2).wait_recv())
        gather_core(c).start()

    def pack(c):
        @pl.loop(0, sources)
        def _(rel):
            s = source_of(rel)
            iota = lax.broadcasted_iota(jnp.int32, (cap, tok), 0)
            one_hot = jnp.where(slot_row[pl.ds(s, 1), :] == iota, 1.0, 0.0).astype(jnp.bfloat16)
            block = g_buf[c, rel // 8, rel // 4 % 2, rel // 2 % 2, rel % 2]
            packed = jnp.dot(one_hot, block, preferred_element_type=jnp.float32)
            pair[0, pl.ds(pl.multiple_of(s * cap, cap), cap), :] = packed.astype(jnp.bfloat16)

    def up_project(c, e0, e1):
        @pl.loop(e0, e1)
        def _(e):
            i = c * experts + e
            for copy in w13_copies(i):
                copy.wait()
            erows = pl.ds(pl.multiple_of(e * per_expert, per_expert), per_expert)
            x_exp[...] = jnp.dot(sel[erows, :], pair[0], preferred_element_type=jnp.float32).astype(jnp.bfloat16)
            for j in range(2):
                prod = jnp.dot(x_exp[...], w13[i % 2, j], preferred_element_type=jnp.float32)

                @pl.when(c == 0)
                def _():
                    acc[j, erows, :] = prod

                @pl.when(c > 0)
                def _():
                    acc[j, erows, :] += prod

            @pl.when(i + 2 < chunks * experts)
            def _():
                for copy in w13_copies(i + 2):
                    copy.start()

    def build_pick():
        tile = 128

        @pl.loop(0, rows // tile)
        def _(t):
            e = t * tile // per_expert
            iota = lax.broadcasted_iota(jnp.int32, (tile, rows), 0) + t * tile % per_expert
            mask = rank_row[pl.ds(e, 1), :] == iota
            trows = pl.ds(pl.multiple_of(t * tile, tile), tile)
            sel[trows, :] = jnp.where(mask, 1.0, 0.0).astype(jnp.bfloat16)
            gate_col[trows, :] = jnp.sum(jnp.where(mask, gate_row[pl.ds(e, 1), :], 0.0), axis=1, keepdims=True)

    start_first(0)
    start_first(1)
    advance(0, 1)
    start_first(2)
    advance(1, 1)
    advance(0, 2)
    build_pick()
    start_first(3)
    advance(2, 1)
    advance(1, 2)
    to_core(0)

    @pl.loop(1, chunks + 1)
    def _(k):
        @pl.when(k + 3 < chunks)
        def _():
            start_first(k + 3)

        @pl.when(k + 2 < chunks)
        def _():
            advance(k + 2, 1)

        @pl.when(k + 1 < chunks)
        def _():
            advance(k + 1, 2)

        gather_core(k - 1).wait_recv()
        pack(k - 1)
        up_project(k - 1, 0, experts // 2)

        @pl.when(k < chunks)
        def _():
            to_core(k)

        up_project(k - 1, experts // 2, experts)

    @pl.loop(0, chunks)
    def _(c):
        for p in PARTS:
            for step in range(3):
                gather_copy(c, p, step).wait_send()
        gather_core(c).wait_send()

    for peer in peers.values():
        pl.semaphore_signal(ready, inc=1, device_id=peer, device_id_type=MESH)

    @pl.loop(0, rows // 128)
    def _(t):
        trows = pl.ds(pl.multiple_of(t * 128, 128), 128)
        hid[trows, :] = (jax.nn.silu(acc[0, trows, :]) * acc[1, trows, :]).astype(jnp.bfloat16)
        iota = lax.broadcasted_iota(jnp.int32, (128, per_expert), 1)
        for e in range(experts):
            mask = rank_col[trows, e:e + 1] == iota
            sel[trows, e * per_expert:(e + 1) * per_expert] = jnp.where(mask, 1.0, 0.0).astype(jnp.bfloat16)

    res_copy.wait()
    pl.semaphore_wait(ready, len(peers))

    def add_into(dst, others):
        total = dst[...].astype(jnp.float32)
        for other in others:
            total = total + other[...].astype(jnp.float32)
        dst[...] = total.astype(jnp.bfloat16)

    def sum_core(k):
        scatter_core(k).wait_recv()

        @pl.loop(0, 8)
        def _(j):
            idx = (j // 4, j // 2 % 2, j % 2)
            add_into(g_buf.at[(k, 0) + idx], [dense.at[(k % 2, 0) + idx]])

    def sum_first(k):
        for p in PARTS:
            scatter_copy(k, p, 0).wait_recv()
            r0, n = ROW_PARTS[p]
            add_into(g_buf.at[(k, 0) + SCATTER_STEPS[p][0][2] + (pl.ds(r0, n),)], [g_buf.at[(k,) + LANDING[0] + (pl.ds(r0, n),)]])

    def sum_second(k):
        for p in PARTS:
            scatter_copy(k, p, 1).wait_recv()
            r0, n = ROW_PARTS[p]
            add_into(g_buf.at[(k, 0) + SCATTER_STEPS[p][2][1] + (pl.ds(r0, n),)], [g_buf.at[k, 1, 1, 0, 1, pl.ds(r0, n)]])

    def finish(k):
        for p in PARTS:
            scatter_copy(k, p, 2).wait_recv()
        cols = pl.ds(pl.multiple_of(k * CW, CW), CW)
        moe = g_buf[k, 0, 0, 0, 0].astype(jnp.float32) + g_buf[k, 1, 1, 0, 0].astype(jnp.float32) + g_buf[k, 1, 1, 1, 0].astype(jnp.float32)
        out_ref[:, cols] = (x_res[:, cols].astype(jnp.float32) + moe).astype(jnp.bfloat16)

    def down_project(k):
        @pl.loop(0, experts)
        def _(e):
            i = k * experts + e
            w2_copy(i).wait()
            erows = pl.ds(pl.multiple_of(e * per_expert, per_expert), per_expert)
            o = jnp.dot(hid[erows, :], w2[i % 2], preferred_element_type=jnp.float32) * gate_col[erows, :]
            hi = o.astype(jnp.bfloat16)
            pair[0, erows, :] = hi
            pair[1, erows, :] = (o - hi.astype(jnp.float32)).astype(jnp.bfloat16)

            @pl.when(i + 2 < chunks * experts)
            def _():
                w2_copy(i + 2).start()

    def combine(k):
        @pl.loop(0, sources // 2)
        def _(m):
            mrows = pl.ds(pl.multiple_of(m * 2 * cap, 2 * cap), 2 * cap)
            pick = sel[mrows, :]
            part = jnp.dot(pick, pair[0], preferred_element_type=jnp.float32)
            part = part + jnp.dot(pick, pair[1], preferred_element_type=jnp.float32)
            part = part.astype(jnp.bfloat16)
            rz, ry, rx = xor(m // 4, zb), xor(m // 2 % 2, yb), xor(m % 2, xb)
            for core in range(2):
                s = m * 2 + core
                slots = slot_col[pl.ds(pl.multiple_of(s * tok, tok), tok), :]
                place = jnp.where(slots == lax.broadcasted_iota(jnp.int32, (tok, cap), 1), 1.0, 0.0).astype(jnp.bfloat16)
                spread = jnp.dot(place, part[core * cap:(core + 1) * cap, :], preferred_element_type=jnp.float32)
                dense[k % 2, xor(core, cb), rz, ry, rx] = spread.astype(jnp.bfloat16)

    @pl.loop(0, chunks + 4)
    def _(k):
        @pl.when((k >= 1) & (k <= chunks))
        def _():
            sum_core(k - 1)

        @pl.when((k >= 2) & (k <= chunks + 1))
        def _():
            sum_first(k - 2)

        @pl.when((k >= 3) & (k <= chunks + 2))
        def _():
            sum_second(k - 3)

        @pl.when((k >= 1) & (k <= chunks))
        def _():
            each(PARTS, lambda p: scatter_copy(k - 1, p, 0).start())

        @pl.when((k >= 2) & (k <= chunks + 1))
        def _():
            each(PARTS, lambda p: scatter_copy(k - 2, p, 1).start())

        @pl.when((k >= 3) & (k <= chunks + 2))
        def _():
            each(PARTS, lambda p: scatter_copy(k - 3, p, 2).start())

        @pl.when(k >= 4)
        def _():
            finish(k - 4)

        @pl.when(k < chunks)
        def _():
            down_project(k)

            @pl.when(k >= 2)
            def _():
                scatter_core(k - 2).wait_send()

            combine(k)
            scatter_core(k).start()

    for k in (chunks - 2, chunks - 1):
        scatter_core(k).wait_send()

    @pl.loop(0, chunks)
    def _(k):
        for p in PARTS:
            for step in range(3):
                scatter_copy(k, p, step).wait_send()


def moe_call(tokens, slot_row, slot_col, rank_row, rank_col, gate_row, w_gate, w_up, w_down):
    tok, hidden = tokens.shape
    experts, _, ff = w_gate.shape
    rows = rank_col.shape[0]
    chunks = hidden // CW
    bf16, f32 = jnp.bfloat16, jnp.float32
    vmem = pl.BlockSpec(memory_space=pltpu.VMEM)
    hbm = pl.BlockSpec(memory_space=pl.ANY)
    dma = pltpu.SemaphoreType.DMA
    return pl.pallas_call(
        moe_kernel,
        out_shape=jax.ShapeDtypeStruct((tok, hidden), bf16),
        in_specs=[hbm, vmem, vmem, vmem, vmem, vmem, hbm, hbm, hbm],
        out_specs=vmem,
        scratch_shapes=[
            pltpu.VMEM((chunks, 2, 2, 2, 2, tok, CW), bf16),
            pltpu.VMEM((2, rows, ff), f32),
            pltpu.VMEM((rows, rows), bf16),
            pltpu.VMEM((2, 2, 2, 2, 2, tok, CW), bf16),
            pltpu.VMEM((rows, ff), bf16),
            pltpu.VMEM((2, 2, CW, ff), bf16),
            pltpu.VMEM((2, ff, CW), bf16),
            pltpu.VMEM((2, rows, CW), bf16),
            pltpu.VMEM((rows // experts, CW), bf16),
            pltpu.VMEM((tok, hidden), bf16),
            pltpu.VMEM((rows, 1), f32),
            dma((chunks, 3, 3)), dma((chunks, 3, 3)), dma((chunks,)), dma((chunks,)), dma((chunks,)),
            dma((2, 2)), dma((2,)), dma, pltpu.SemaphoreType.REGULAR,
        ],
        compiler_params=pltpu.CompilerParams(collective_id=0, has_side_effects=True, vmem_limit_bytes=67043328),
    )(tokens, slot_row, slot_col, rank_row, rank_col, gate_row, w_gate, w_up, w_down)


def solution(mesh):
    ep_axes = tuple(mesh.axis_names)
    num_devices = math.prod(mesh.shape[axis_name] for axis_name in ep_axes)
    row_spec = P(ep_axes, None)
    w_spec = P(ep_axes, None, None)

    def local_layer(tokens, expert_ids, gate_weights, w_gate, w_up, w_down):
        tok_dev, hidden = tokens.shape
        top_k = expert_ids.shape[1]
        local_experts = w_gate.shape[0]
        capacity = tok_dev * top_k // num_devices
        rows = num_devices * capacity
        all_experts = jnp.arange(num_devices * local_experts)
        gate_dense = jnp.sum(jnp.where(expert_ids[:, :, None] == all_experts[None, None, :], gate_weights[:, :, None], 0.0), axis=1)
        gate_send = gate_dense.reshape(tok_dev, num_devices, local_experts).transpose(1, 2, 0)
        gates = lax.all_to_all(gate_send, ep_axes, 0, 0, tiled=True)
        hit = jnp.any(gates > 0.0, axis=1)
        slot = jnp.where(hit, jnp.cumsum(hit.astype(jnp.int32), axis=1) - 1, -1)
        place = slot[:, None, :] == jnp.arange(capacity)[None, :, None]
        gate_pack = jnp.sum(jnp.where(place[:, None], gates[:, :, None, :], 0.0), axis=3)
        gate_pack = gate_pack.transpose(1, 0, 2).reshape(local_experts, rows)
        chosen = gate_pack > 0.0
        rank = jnp.where(chosen, jnp.cumsum(chosen.astype(jnp.int32), axis=1) - 1, -1)
        return moe_call(tokens, slot, slot.reshape(-1, 1), rank, rank.T, gate_pack, w_gate, w_up, w_down)

    return jax.shard_map(local_layer, mesh=mesh, in_specs=(row_spec, row_spec, row_spec, w_spec, w_spec, w_spec), out_specs=row_spec, check_vma=False)
```

```python
import math
import jax
import jax.numpy as jnp
from jax import lax
from jax.experimental import pallas as pl
from jax.experimental.pallas import tpu as pltpu
from jax.sharding import PartitionSpec as P

MESH = pl.DeviceIdType.MESH
CW = 256
ROW_PARTS = ((0, 96), (96, 80), (176, 80))
ALL = slice(None)
GATHER_STEPS = (
    (("x", (0, 0, 0), (0, 0, 1)), ("y", (0, 0, ALL), (0, 1, ALL)), ("z", (0, ALL, ALL), (1, ALL, ALL))),
    (("y", (0, 0, 0), (0, 1, 0)), ("z", (0, ALL, 0), (1, ALL, 0)), ("x", (ALL, ALL, 0), (ALL, ALL, 1))),
    (("z", (0, 0, 0), (1, 0, 0)), ("x", (ALL, 0, 0), (ALL, 0, 1)), ("y", (ALL, 0, ALL), (ALL, 1, ALL))),
)
SCATTER_STEPS = tuple(tuple((link, dst, src) for link, src, dst in steps[::-1]) for steps in GATHER_STEPS)
LANDING = ((1, 0, ALL, ALL), (1, 1, 0, ALL), (1, 1, 1, 0))


def moe_kernel(x_hbm, slot_row, slot_col, rank_row, rank_col, gate_row, w1_hbm, w3_hbm, w2_hbm, out_ref,
               g_buf, acc, sel, dense, hid, w13, w2, pair, x_exp, x_res, gate_col,
               step_send, step_recv, core_send, core_recv, x_sem, w13_sem, w2_sem, res_sem, ready):
    zb, yb, ex = lax.axis_index("ez"), lax.axis_index("ey"), lax.axis_index("ex")
    xb, cb = ex // 2, ex % 2
    peers = {
        "x": (zb, yb, (1 - xb) * 2 + cb),
        "y": (zb, 1 - yb, ex),
        "z": (1 - zb, yb, ex),
        "core": (zb, yb, xb * 2 + 1 - cb),
    }
    tok = x_hbm.shape[0]
    hidden = x_hbm.shape[1]
    chunks = hidden // CW
    experts, _, ff = w1_hbm.shape
    sources = slot_row.shape[0]
    rows = rank_col.shape[0]
    cap = rows // sources
    per_expert = rows // experts

    def xor(a, b):
        return a + b - 2 * a * b

    def source_of(rel):
        return (xor(zb, rel // 4 % 2) * 8 + xor(yb, rel // 2 % 2) * 4 + xor(xb, rel % 2) * 2 + xor(cb, rel // 8))

    def gather_copy(c, part, step):
        r0, n = ROW_PARTS[part]
        link, src, dst = GATHER_STEPS[part][step]
        return pltpu.make_async_remote_copy(
            g_buf.at[(c, 0) + src + (pl.ds(r0, n),)], g_buf.at[(c, 0) + dst + (pl.ds(r0, n),)],
            step_send.at[c, part, step], step_recv.at[c, part, step], device_id=peers[link], device_id_type=MESH)

    def gather_core(c):
        return pltpu.make_async_remote_copy(g_buf.at[c, 0], g_buf.at[c, 1], core_send.at[c], core_recv.at[c],
                                            device_id=peers["core"], device_id_type=MESH)

    def scatter_core(k):
        return pltpu.make_async_remote_copy(dense.at[k % 2, 1], g_buf.at[k, 0], core_send.at[k], core_recv.at[k],
                                            device_id=peers["core"], device_id_type=MESH)

    def scatter_copy(k, part, step):
        r0, n = ROW_PARTS[part]
        link, src, _ = SCATTER_STEPS[part][step]
        return pltpu.make_async_remote_copy(
            g_buf.at[(k, 0) + src + (pl.ds(r0, n),)], g_buf.at[(k,) + LANDING[step] + (pl.ds(r0, n),)],
            step_send.at[k, part, step], step_recv.at[k, part, step], device_id=peers[link], device_id_type=MESH)

    def x_copy(c):
        cols = pl.ds(pl.multiple_of(c * CW, CW), CW)
        return pltpu.make_async_copy(x_hbm.at[:, cols], g_buf.at[c, 0, 0, 0, 0], x_sem.at[c])

    def w13_copies(i):
        c, e, b = i // experts, i % experts, i % 2
        k_rows = pl.ds(pl.multiple_of(c * CW, CW), CW)
        return (pltpu.make_async_copy(w1_hbm.at[e, k_rows], w13.at[b, 0], w13_sem.at[b, 0]),
                pltpu.make_async_copy(w3_hbm.at[e, k_rows], w13.at[b, 1], w13_sem.at[b, 1]))

    def w2_copy(i):
        k, e, b = i // experts, i % experts, i % 2
        cols = pl.ds(pl.multiple_of(k * CW, CW), CW)
        return pltpu.make_async_copy(w2_hbm.at[e, :, cols], w2.at[b], w2_sem.at[b])

    def each(parts, fn):
        for part in parts:
            fn(part)

    PARTS = range(len(ROW_PARTS))

    for c in range(chunks):
        x_copy(c).start()
    res_copy = pltpu.make_async_copy(x_hbm, x_res, res_sem)
    res_copy.start()
    for i in range(2):
        for copy in w13_copies(i):
            copy.start()
        w2_copy(i).start()
    barrier = pltpu.get_barrier_semaphore()
    for peer in peers.values():
        pl.semaphore_signal(barrier, inc=1, device_id=peer, device_id_type=MESH)
    pl.semaphore_wait(barrier, len(peers))

    @jax.named_scope("start_first")
    def start_first(c):
        x_copy(c).wait()
        each(PARTS, lambda p: gather_copy(c, p, 0).start())

    @jax.named_scope("advance")
    def advance(c, step):
        def one(p):
            gather_copy(c, p, step - 1).wait_recv()
            gather_copy(c, p, step).start()
        each(PARTS, one)

    @jax.named_scope("to_core")
    def to_core(c):
        each(PARTS, lambda p: gather_copy(c, p, 2).wait_recv())
        gather_core(c).start()

    @jax.named_scope("pack")
    def pack(c):
        @pl.loop(0, sources)
        def _(rel):
            s = source_of(rel)
            iota = lax.broadcasted_iota(jnp.int32, (cap, tok), 0)
            one_hot = jnp.where(slot_row[pl.ds(s, 1), :] == iota, 1.0, 0.0).astype(jnp.bfloat16)
            block = g_buf[c, rel // 8, rel // 4 % 2, rel // 2 % 2, rel % 2]
            packed = jnp.dot(one_hot, block, preferred_element_type=jnp.float32)
            pair[0, pl.ds(pl.multiple_of(s * cap, cap), cap), :] = packed.astype(jnp.bfloat16)

    @jax.named_scope("up_project")
    def up_project(c, e0, e1):
        @pl.loop(e0, e1)
        def _(e):
            i = c * experts + e
            for copy in w13_copies(i):
                copy.wait()
            erows = pl.ds(pl.multiple_of(e * per_expert, per_expert), per_expert)
            x_exp[...] = jnp.dot(sel[erows, :], pair[0], preferred_element_type=jnp.float32).astype(jnp.bfloat16)
            for j in range(2):
                for n in range(0, ff, CW):
                    acc[j, erows, n:n + CW] += jnp.dot(x_exp[...], w13[i % 2, j, :, n:n + CW], preferred_element_type=jnp.float32)

            @pl.when(i + 2 < chunks * experts)
            def _():
                for copy in w13_copies(i + 2):
                    copy.start()

    @jax.named_scope("build_pick")
    def build_pick():
        tile = 128

        @pl.loop(0, rows // tile)
        def _(t):
            e = t * tile // per_expert
            iota = lax.broadcasted_iota(jnp.int32, (tile, rows), 0) + t * tile % per_expert
            mask = rank_row[pl.ds(e, 1), :] == iota
            trows = pl.ds(pl.multiple_of(t * tile, tile), tile)
            sel[trows, :] = jnp.where(mask, 1.0, 0.0).astype(jnp.bfloat16)
            gate_col[trows, :] = jnp.sum(jnp.where(mask, gate_row[pl.ds(e, 1), :], 0.0), axis=1, keepdims=True)

    @jax.named_scope("clear_sums")
    def clear_sums():
        @pl.loop(0, rows // 64)
        def _(t):
            trows = pl.ds(pl.multiple_of(t * 64, 64), 64)
            for j in range(2):
                acc[j, trows, :] = jnp.zeros((64, ff), jnp.float32)

    start_first(0)
    start_first(1)
    clear_sums()
    advance(0, 1)
    start_first(2)
    build_pick()
    advance(1, 1)
    advance(0, 2)
    start_first(3)
    advance(2, 1)
    advance(1, 2)
    to_core(0)

    @pl.loop(1, chunks + 1)
    def _(k):
        @pl.when(k + 3 < chunks)
        def _():
            start_first(k + 3)

        @pl.when(k + 2 < chunks)
        def _():
            advance(k + 2, 1)

        @pl.when(k + 1 < chunks)
        def _():
            advance(k + 1, 2)

        gather_core(k - 1).wait_recv()
        pack(k - 1)
        up_project(k - 1, 0, experts // 2)

        @pl.when(k < chunks)
        def _():
            to_core(k)

        up_project(k - 1, experts // 2, experts)

    @pl.loop(0, chunks)
    def _(c):
        for p in PARTS:
            for step in range(3):
                gather_copy(c, p, step).wait_send()
        gather_core(c).wait_send()

    for peer in peers.values():
        pl.semaphore_signal(ready, inc=1, device_id=peer, device_id_type=MESH)

    @pl.loop(0, rows // 128)
    def _(t):
        trows = pl.ds(pl.multiple_of(t * 128, 128), 128)
        hid[trows, :] = (jax.nn.silu(acc[0, trows, :]) * acc[1, trows, :]).astype(jnp.bfloat16)
        iota = lax.broadcasted_iota(jnp.int32, (128, per_expert), 1)
        for e in range(experts):
            mask = rank_col[trows, e:e + 1] == iota
            sel[trows, e * per_expert:(e + 1) * per_expert] = jnp.where(mask, 1.0, 0.0).astype(jnp.bfloat16)

    res_copy.wait()
    pl.semaphore_wait(ready, len(peers))

    def add_into(dst, others):
        total = dst[...].astype(jnp.float32)
        for other in others:
            total = total + other[...].astype(jnp.float32)
        dst[...] = total.astype(jnp.bfloat16)

    @jax.named_scope("sum_core")
    def sum_core(k):
        scatter_core(k).wait_recv()

        @pl.loop(0, 8)
        def _(j):
            idx = (j // 4, j // 2 % 2, j % 2)
            add_into(g_buf.at[(k, 0) + idx], [dense.at[(k % 2, 0) + idx]])

    @jax.named_scope("sum_first")
    def sum_first(k):
        for p in PARTS:
            scatter_copy(k, p, 0).wait_recv()
            r0, n = ROW_PARTS[p]
            add_into(g_buf.at[(k, 0) + SCATTER_STEPS[p][0][2] + (pl.ds(r0, n),)], [g_buf.at[(k,) + LANDING[0] + (pl.ds(r0, n),)]])

    @jax.named_scope("sum_second")
    def sum_second(k):
        for p in PARTS:
            scatter_copy(k, p, 1).wait_recv()
            r0, n = ROW_PARTS[p]
            add_into(g_buf.at[(k, 0) + SCATTER_STEPS[p][2][1] + (pl.ds(r0, n),)], [g_buf.at[k, 1, 1, 0, 1, pl.ds(r0, n)]])

    @jax.named_scope("finish")
    def finish(k):
        for p in PARTS:
            scatter_copy(k, p, 2).wait_recv()
        cols = pl.ds(pl.multiple_of(k * CW, CW), CW)
        moe = g_buf[k, 0, 0, 0, 0].astype(jnp.float32) + g_buf[k, 1, 1, 0, 0].astype(jnp.float32) + g_buf[k, 1, 1, 1, 0].astype(jnp.float32)
        out_ref[:, cols] = (x_res[:, cols].astype(jnp.float32) + moe).astype(jnp.bfloat16)

    def start_scatter(k):
        each(PARTS, lambda p: scatter_copy(k, p, 0).start())

    @jax.named_scope("down_project")
    def down_project(k):
        @pl.loop(0, experts)
        def _(e):
            i = k * experts + e
            w2_copy(i).wait()
            erows = pl.ds(pl.multiple_of(e * per_expert, per_expert), per_expert)
            o = jnp.dot(hid[erows, :], w2[i % 2], preferred_element_type=jnp.float32) * gate_col[erows, :]
            hi = o.astype(jnp.bfloat16)
            pair[0, erows, :] = hi
            pair[1, erows, :] = (o - hi.astype(jnp.float32)).astype(jnp.bfloat16)

            @pl.when(i + 2 < chunks * experts)
            def _():
                w2_copy(i + 2).start()

    @jax.named_scope("combine")
    def combine(k):
        @pl.loop(0, sources // 2)
        def _(m):
            @pl.when((m == 1) & (k >= 1))
            def _():
                start_scatter(k - 1)

            mrows = pl.ds(pl.multiple_of(m * 2 * cap, 2 * cap), 2 * cap)
            pick = sel[mrows, :]
            part = jnp.dot(pick, pair[0], preferred_element_type=jnp.float32)
            part = part + jnp.dot(pick, pair[1], preferred_element_type=jnp.float32)
            part = part.astype(jnp.bfloat16)
            rz, ry, rx = xor(m // 4, zb), xor(m // 2 % 2, yb), xor(m % 2, xb)
            for core in range(2):
                s = m * 2 + core
                slots = slot_col[pl.ds(pl.multiple_of(s * tok, tok), tok), :]
                place = jnp.where(slots == lax.broadcasted_iota(jnp.int32, (tok, cap), 1), 1.0, 0.0).astype(jnp.bfloat16)
                spread = jnp.dot(place, part[core * cap:(core + 1) * cap, :], preferred_element_type=jnp.float32)
                dense[k % 2, xor(core, cb), rz, ry, rx] = spread.astype(jnp.bfloat16)

    @pl.loop(0, chunks + 4)
    def _(k):
        @pl.when((k >= 2) & (k <= chunks + 1))
        def _():
            sum_first(k - 2)

        @pl.when((k >= 3) & (k <= chunks + 2))
        def _():
            sum_second(k - 3)

        @pl.when((k >= 2) & (k <= chunks + 1))
        def _():
            each(PARTS, lambda p: scatter_copy(k - 2, p, 1).start())

        @pl.when((k >= 3) & (k <= chunks + 2))
        def _():
            each(PARTS, lambda p: scatter_copy(k - 3, p, 2).start())

        @pl.when(k < chunks)
        def _():
            down_project(k)

        @pl.when((k >= 1) & (k <= chunks))
        def _():
            sum_core(k - 1)

        @pl.when(k == chunks)
        def _():
            start_scatter(k - 1)

        @pl.when(k < chunks)
        def _():
            @pl.when(k >= 2)
            def _():
                scatter_core(k - 2).wait_send()

            combine(k)
            scatter_core(k).start()

        @pl.when(k >= 4)
        def _():
            finish(k - 4)

    for k in (chunks - 2, chunks - 1):
        scatter_core(k).wait_send()

    @pl.loop(0, chunks)
    def _(k):
        for p in PARTS:
            for step in range(3):
                scatter_copy(k, p, step).wait_send()


def moe_call(tokens, slot_row, slot_col, rank_row, rank_col, gate_row, w_gate, w_up, w_down):
    tok, hidden = tokens.shape
    experts, _, ff = w_gate.shape
    rows = rank_col.shape[0]
    chunks = hidden // CW
    bf16, f32 = jnp.bfloat16, jnp.float32
    vmem = pl.BlockSpec(memory_space=pltpu.VMEM)
    hbm = pl.BlockSpec(memory_space=pl.ANY)
    dma = pltpu.SemaphoreType.DMA
    return pl.pallas_call(
        moe_kernel,
        out_shape=jax.ShapeDtypeStruct((tok, hidden), bf16),
        in_specs=[hbm, vmem, vmem, vmem, vmem, vmem, hbm, hbm, hbm],
        out_specs=vmem,
        scratch_shapes=[
            pltpu.VMEM((chunks, 2, 2, 2, 2, tok, CW), bf16),
            pltpu.VMEM((2, rows, ff), f32),
            pltpu.VMEM((rows, rows), bf16),
            pltpu.VMEM((2, 2, 2, 2, 2, tok, CW), bf16),
            pltpu.VMEM((rows, ff), bf16),
            pltpu.VMEM((2, 2, CW, ff), bf16),
            pltpu.VMEM((2, ff, CW), bf16),
            pltpu.VMEM((2, rows, CW), bf16),
            pltpu.VMEM((rows // experts, CW), bf16),
            pltpu.VMEM((tok, hidden), bf16),
            pltpu.VMEM((rows, 1), f32),
            dma((chunks, 3, 3)), dma((chunks, 3, 3)), dma((chunks,)), dma((chunks,)), dma((chunks,)),
            dma((2, 2)), dma((2,)), dma, pltpu.SemaphoreType.REGULAR,
        ],
        compiler_params=pltpu.CompilerParams(collective_id=0, has_side_effects=True, vmem_limit_bytes=67043328),
    )(tokens, slot_row, slot_col, rank_row, rank_col, gate_row, w_gate, w_up, w_down)


def solution(mesh):
    ep_axes = tuple(mesh.axis_names)
    num_devices = math.prod(mesh.shape[axis_name] for axis_name in ep_axes)
    row_spec = P(ep_axes, None)
    w_spec = P(ep_axes, None, None)

    def local_layer(tokens, expert_ids, gate_weights, w_gate, w_up, w_down):
        tok_dev, hidden = tokens.shape
        top_k = expert_ids.shape[1]
        local_experts = w_gate.shape[0]
        capacity = tok_dev * top_k // num_devices
        rows = num_devices * capacity
        all_experts = jnp.arange(num_devices * local_experts)
        gate_dense = jnp.sum(jnp.where(expert_ids[:, :, None] == all_experts[None, None, :], gate_weights[:, :, None], 0.0), axis=1)
        gate_send = gate_dense.reshape(tok_dev, num_devices, local_experts).transpose(1, 2, 0)
        gates = lax.all_to_all(gate_send, ep_axes, 0, 0, tiled=True)
        hit = jnp.any(gates > 0.0, axis=1)
        slot = jnp.where(hit, jnp.cumsum(hit.astype(jnp.int32), axis=1) - 1, -1)
        place = slot[:, None, :] == jnp.arange(capacity)[None, :, None]
        gate_pack = jnp.sum(jnp.where(place[:, None], gates[:, :, None, :], 0.0), axis=3)
        gate_pack = gate_pack.transpose(1, 0, 2).reshape(local_experts, rows)
        chosen = gate_pack > 0.0
        rank = jnp.where(chosen, jnp.cumsum(chosen.astype(jnp.int32), axis=1) - 1, -1)
        return moe_call(tokens, slot, slot.reshape(-1, 1), rank, rank.T, gate_pack, w_gate, w_up, w_down)

    return jax.shard_map(local_layer, mesh=mesh, in_specs=(row_spec, row_spec, row_spec, w_spec, w_spec, w_spec), out_specs=row_spec, check_vma=False)
```

```python
import math
import jax
import jax.numpy as jnp
from jax import lax
from jax.experimental import pallas as pl
from jax.experimental.pallas import tpu as pltpu
from jax.sharding import PartitionSpec as P

MESH = pl.DeviceIdType.MESH
CW = 256
ROW_PARTS = ((0, 96), (96, 80), (176, 80))
ALL = slice(None)
GATHER_STEPS = (
    (("x", (0, 0, 0), (0, 0, 1)), ("y", (0, 0, ALL), (0, 1, ALL)), ("z", (0, ALL, ALL), (1, ALL, ALL))),
    (("y", (0, 0, 0), (0, 1, 0)), ("z", (0, ALL, 0), (1, ALL, 0)), ("x", (ALL, ALL, 0), (ALL, ALL, 1))),
    (("z", (0, 0, 0), (1, 0, 0)), ("x", (ALL, 0, 0), (ALL, 0, 1)), ("y", (ALL, 0, ALL), (ALL, 1, ALL))),
)
SCATTER_STEPS = tuple(tuple((link, dst, src) for link, src, dst in steps[::-1]) for steps in GATHER_STEPS)
LANDING = ((1, 0, ALL, ALL), (1, 1, 0, ALL), (1, 1, 1, 0))


def moe_kernel(x_hbm, slot_row, slot_col, rank_row, rank_col, gate_row, w1_hbm, w3_hbm, w2_hbm, out_ref,
               g_buf, acc, sel, dense, hid, w13, w2, pair, x_exp, part, x_res, gate_col,
               step_send, step_recv, core_send, core_recv, x_sem, w13_sem, w2_sem, res_sem, ready):
    zb, yb, ex = lax.axis_index("ez"), lax.axis_index("ey"), lax.axis_index("ex")
    xb, cb = ex // 2, ex % 2
    peers = {
        "x": (zb, yb, (1 - xb) * 2 + cb),
        "y": (zb, 1 - yb, ex),
        "z": (1 - zb, yb, ex),
        "core": (zb, yb, xb * 2 + 1 - cb),
    }
    tok = x_hbm.shape[0]
    hidden = x_hbm.shape[1]
    chunks = hidden // CW
    experts, _, ff = w1_hbm.shape
    sources = slot_row.shape[0]
    rows = rank_col.shape[0]
    cap = rows // sources
    per_expert = rows // experts

    def xor(a, b):
        return a + b - 2 * a * b

    def source_of(rel):
        return (xor(zb, rel // 4 % 2) * 8 + xor(yb, rel // 2 % 2) * 4 + xor(xb, rel % 2) * 2 + xor(cb, rel // 8))

    def gather_copy(c, part, step):
        r0, n = ROW_PARTS[part]
        link, src, dst = GATHER_STEPS[part][step]
        return pltpu.make_async_remote_copy(
            g_buf.at[(c, 0) + src + (pl.ds(r0, n),)], g_buf.at[(c, 0) + dst + (pl.ds(r0, n),)],
            step_send.at[c, part, step], step_recv.at[c, part, step], device_id=peers[link], device_id_type=MESH)

    def gather_core(c):
        return pltpu.make_async_remote_copy(g_buf.at[c, 0], g_buf.at[c, 1], core_send.at[c], core_recv.at[c],
                                            device_id=peers["core"], device_id_type=MESH)

    def scatter_core(k):
        return pltpu.make_async_remote_copy(dense.at[k % 2, 1], g_buf.at[k, 0], core_send.at[k], core_recv.at[k],
                                            device_id=peers["core"], device_id_type=MESH)

    def scatter_copy(k, part, step):
        r0, n = ROW_PARTS[part]
        link, src, _ = SCATTER_STEPS[part][step]
        return pltpu.make_async_remote_copy(
            g_buf.at[(k, 0) + src + (pl.ds(r0, n),)], g_buf.at[(k,) + LANDING[step] + (pl.ds(r0, n),)],
            step_send.at[k, part, step], step_recv.at[k, part, step], device_id=peers[link], device_id_type=MESH)

    def x_copy(c):
        cols = pl.ds(pl.multiple_of(c * CW, CW), CW)
        return pltpu.make_async_copy(x_hbm.at[:, cols], g_buf.at[c, 0, 0, 0, 0], x_sem.at[c])

    def w13_copies(c, e):
        b = e % 2
        k_rows = pl.ds(pl.multiple_of(c * CW, CW), CW)
        return (pltpu.make_async_copy(w1_hbm.at[e, k_rows], w13.at[b, 0], w13_sem.at[b, 0]),
                pltpu.make_async_copy(w3_hbm.at[e, k_rows], w13.at[b, 1], w13_sem.at[b, 1]))

    def w2_copy(k, e):
        cols = pl.ds(pl.multiple_of(k * CW, CW), CW)
        return pltpu.make_async_copy(w2_hbm.at[e, :, cols], w2.at[e % 2], w2_sem.at[e % 2])

    def each(parts, fn):
        for part in parts:
            fn(part)

    PARTS = range(len(ROW_PARTS))

    for c in range(chunks):
        x_copy(c).start()
    res_copy = pltpu.make_async_copy(x_hbm, x_res, res_sem)
    res_copy.start()
    for e in range(2):
        for copy in w13_copies(0, e):
            copy.start()
        w2_copy(0, e).start()
    barrier = pltpu.get_barrier_semaphore()
    for peer in peers.values():
        pl.semaphore_signal(barrier, inc=1, device_id=peer, device_id_type=MESH)
    pl.semaphore_wait(barrier, len(peers))

    @jax.named_scope("start_first")
    def start_first(c):
        x_copy(c).wait()
        each(PARTS, lambda p: gather_copy(c, p, 0).start())

    @jax.named_scope("advance")
    def advance(c, step):
        def one(p):
            gather_copy(c, p, step - 1).wait_recv()
            gather_copy(c, p, step).start()
        each(PARTS, one)

    @jax.named_scope("to_core")
    def to_core(c):
        each(PARTS, lambda p: gather_copy(c, p, 2).wait_recv())
        gather_core(c).start()

    @jax.named_scope("pack")
    def pack(c):
        @pl.loop(0, sources // 4)
        def _(q):
            for u in range(4):
                rel = q * 4 + u
                s = source_of(rel)
                iota = lax.broadcasted_iota(jnp.int32, (cap, tok), 0)
                one_hot = jnp.where(slot_row[pl.ds(s, 1), :] == iota, 1.0, 0.0).astype(jnp.bfloat16)
                block = g_buf[c, rel // 8, rel // 4 % 2, rel // 2 % 2, rel % 2]
                packed = jnp.dot(one_hot, block, preferred_element_type=jnp.float32)
                pair[0, pl.ds(pl.multiple_of(s * cap, cap), cap), :] = packed.astype(jnp.bfloat16)

    @jax.named_scope("pick")
    def pick(e):
        x_exp[e % 2] = jnp.dot(sel[e * per_expert:(e + 1) * per_expert, :], pair[0], preferred_element_type=jnp.float32).astype(jnp.bfloat16)

    @jax.named_scope("up_project")
    def up_project(c, e):
        for copy in w13_copies(c, e):
            copy.wait()
        erows = slice(e * per_expert, (e + 1) * per_expert)
        for j in range(2):
            for n in range(0, ff, CW):
                acc[j, erows, n:n + CW] += jnp.dot(x_exp[e % 2], w13[e % 2, j, :, n:n + CW], preferred_element_type=jnp.float32)
        if e + 1 < experts:
            pick(e + 1)
        nc, ne = (c, e + 2) if e + 2 < experts else (c + 1, e + 2 - experts)

        @pl.when(nc < chunks)
        def _():
            for copy in w13_copies(nc, ne):
                copy.start()

    @jax.named_scope("build_pick")
    def build_pick():
        tile = 128

        @pl.loop(0, rows // tile)
        def _(t):
            e = t * tile // per_expert
            iota = lax.broadcasted_iota(jnp.int32, (tile, rows), 0) + t * tile % per_expert
            mask = rank_row[pl.ds(e, 1), :] == iota
            trows = pl.ds(pl.multiple_of(t * tile, tile), tile)
            sel[trows, :] = jnp.where(mask, 1.0, 0.0).astype(jnp.bfloat16)
            gate_col[trows, :] = jnp.sum(jnp.where(mask, gate_row[pl.ds(e, 1), :], 0.0), axis=1, keepdims=True)

    @jax.named_scope("clear_sums")
    def clear_sums():
        @pl.loop(0, rows // 64)
        def _(t):
            trows = pl.ds(pl.multiple_of(t * 64, 64), 64)
            for j in range(2):
                acc[j, trows, :] = jnp.zeros((64, ff), jnp.float32)

    start_first(0)
    start_first(1)
    clear_sums()
    advance(0, 1)
    start_first(2)
    build_pick()
    advance(1, 1)
    advance(0, 2)
    start_first(3)
    advance(2, 1)
    advance(1, 2)
    to_core(0)

    @pl.loop(1, chunks + 1)
    def _(k):
        @pl.when(k + 3 < chunks)
        def _():
            start_first(k + 3)

        @pl.when(k + 2 < chunks)
        def _():
            advance(k + 2, 1)

        @pl.when(k + 1 < chunks)
        def _():
            advance(k + 1, 2)

        gather_core(k - 1).wait_recv()
        pack(k - 1)
        pick(0)
        for e in range(experts // 2):
            up_project(k - 1, e)

        @pl.when(k < chunks)
        def _():
            to_core(k)

        for e in range(experts // 2, experts):
            up_project(k - 1, e)

    @pl.loop(0, chunks)
    def _(c):
        for p in PARTS:
            for step in range(3):
                gather_copy(c, p, step).wait_send()
        gather_core(c).wait_send()

    for peer in peers.values():
        pl.semaphore_signal(ready, inc=1, device_id=peer, device_id_type=MESH)

    @pl.loop(0, rows // 128)
    def _(t):
        trows = pl.ds(pl.multiple_of(t * 128, 128), 128)
        hid[trows, :] = (jax.nn.silu(acc[0, trows, :]) * acc[1, trows, :]).astype(jnp.bfloat16)
        iota = lax.broadcasted_iota(jnp.int32, (128, per_expert), 1)
        for e in range(experts):
            mask = rank_col[trows, e:e + 1] == iota
            sel[trows, e * per_expert:(e + 1) * per_expert] = jnp.where(mask, 1.0, 0.0).astype(jnp.bfloat16)

    res_copy.wait()
    pl.semaphore_wait(ready, len(peers))

    def add_into(dst, others):
        total = dst[...].astype(jnp.float32)
        for other in others:
            total = total + other[...].astype(jnp.float32)
        dst[...] = total.astype(jnp.bfloat16)

    @jax.named_scope("sum_core")
    def sum_core(k):
        scatter_core(k).wait_recv()

        @pl.loop(0, 8)
        def _(j):
            idx = (j // 4, j // 2 % 2, j % 2)
            add_into(g_buf.at[(k, 0) + idx], [dense.at[(k % 2, 0) + idx]])

    @jax.named_scope("sum_first")
    def sum_first(k):
        for p in PARTS:
            scatter_copy(k, p, 0).wait_recv()
            r0, n = ROW_PARTS[p]
            add_into(g_buf.at[(k, 0) + SCATTER_STEPS[p][0][2] + (pl.ds(r0, n),)], [g_buf.at[(k,) + LANDING[0] + (pl.ds(r0, n),)]])

    @jax.named_scope("sum_second")
    def sum_second(k):
        for p in PARTS:
            scatter_copy(k, p, 1).wait_recv()
            r0, n = ROW_PARTS[p]
            add_into(g_buf.at[(k, 0) + SCATTER_STEPS[p][2][1] + (pl.ds(r0, n),)], [g_buf.at[k, 1, 1, 0, 1, pl.ds(r0, n)]])

    @jax.named_scope("finish")
    def finish(k):
        for p in PARTS:
            scatter_copy(k, p, 2).wait_recv()
        cols = pl.ds(pl.multiple_of(k * CW, CW), CW)
        moe = g_buf[k, 0, 0, 0, 0].astype(jnp.float32) + g_buf[k, 1, 1, 0, 0].astype(jnp.float32) + g_buf[k, 1, 1, 1, 0].astype(jnp.float32)
        out_ref[:, cols] = (x_res[:, cols].astype(jnp.float32) + moe).astype(jnp.bfloat16)

    def start_scatter(k):
        each(PARTS, lambda p: scatter_copy(k, p, 0).start())

    @jax.named_scope("down_project")
    def down_project(k):
        for e in range(experts):
            w2_copy(k, e).wait()
            erows = slice(e * per_expert, (e + 1) * per_expert)
            o = jnp.dot(hid[erows, :], w2[e % 2], preferred_element_type=jnp.float32) * gate_col[erows, :]
            hi = o.astype(jnp.bfloat16)
            pair[0, erows, :] = hi
            pair[1, erows, :] = (o - hi.astype(jnp.float32)).astype(jnp.bfloat16)
            nk, ne = (k, e + 2) if e + 2 < experts else (k + 1, e + 2 - experts)

            @pl.when(nk < chunks)
            def _():
                w2_copy(nk, ne).start()

    MT = 4 * cap

    @jax.named_scope("combine")
    def combine(k):
        def gather_sum(m):
            chosen = sel[m * MT:(m + 1) * MT, :]
            total = jnp.dot(chosen, pair[0], preferred_element_type=jnp.float32)
            total = total + jnp.dot(chosen, pair[1], preferred_element_type=jnp.float32)
            part[m % 2] = total.astype(jnp.bfloat16)

        def spread(m):
            for u in range(MT // cap):
                s = m * (MT // cap) + u
                chip, core = s // 2, s % 2
                slots = slot_col[s * tok:(s + 1) * tok, :]
                place = jnp.where(slots == lax.broadcasted_iota(jnp.int32, (tok, cap), 1), 1.0, 0.0).astype(jnp.bfloat16)
                block = jnp.dot(place, part[m % 2, u * cap:(u + 1) * cap, :], preferred_element_type=jnp.float32)
                dense[k % 2, xor(core, cb), xor(chip // 4, zb), xor(chip // 2 % 2, yb), xor(chip % 2, xb)] = block.astype(jnp.bfloat16)

        gather_sum(0)

        @pl.when(k >= 1)
        def _():
            start_scatter(k - 1)

        for m in range(1, rows // MT + 1):
            if m < rows // MT:
                gather_sum(m)
            spread(m - 1)

    @pl.loop(0, chunks + 4)
    def _(k):
        @pl.when((k >= 2) & (k <= chunks + 1))
        def _():
            sum_first(k - 2)

        @pl.when((k >= 3) & (k <= chunks + 2))
        def _():
            sum_second(k - 3)

        @pl.when((k >= 2) & (k <= chunks + 1))
        def _():
            each(PARTS, lambda p: scatter_copy(k - 2, p, 1).start())

        @pl.when((k >= 3) & (k <= chunks + 2))
        def _():
            each(PARTS, lambda p: scatter_copy(k - 3, p, 2).start())

        @pl.when(k < chunks)
        def _():
            down_project(k)

        @pl.when((k >= 1) & (k <= chunks))
        def _():
            sum_core(k - 1)

        @pl.when(k == chunks)
        def _():
            start_scatter(k - 1)

        @pl.when(k < chunks)
        def _():
            @pl.when(k >= 2)
            def _():
                scatter_core(k - 2).wait_send()

            combine(k)
            scatter_core(k).start()

        @pl.when(k >= 4)
        def _():
            finish(k - 4)

    for k in (chunks - 2, chunks - 1):
        scatter_core(k).wait_send()

    @pl.loop(0, chunks)
    def _(k):
        for p in PARTS:
            for step in range(3):
                scatter_copy(k, p, step).wait_send()


def moe_call(tokens, slot_row, slot_col, rank_row, rank_col, gate_row, w_gate, w_up, w_down):
    tok, hidden = tokens.shape
    experts, _, ff = w_gate.shape
    rows = rank_col.shape[0]
    chunks = hidden // CW
    bf16, f32 = jnp.bfloat16, jnp.float32
    vmem = pl.BlockSpec(memory_space=pltpu.VMEM)
    hbm = pl.BlockSpec(memory_space=pl.ANY)
    dma = pltpu.SemaphoreType.DMA
    return pl.pallas_call(
        moe_kernel,
        out_shape=jax.ShapeDtypeStruct((tok, hidden), bf16),
        in_specs=[hbm, vmem, vmem, vmem, vmem, vmem, hbm, hbm, hbm],
        out_specs=vmem,
        scratch_shapes=[
            pltpu.VMEM((chunks, 2, 2, 2, 2, tok, CW), bf16),
            pltpu.VMEM((2, rows, ff), f32),
            pltpu.VMEM((rows, rows), bf16),
            pltpu.VMEM((2, 2, 2, 2, 2, tok, CW), bf16),
            pltpu.VMEM((rows, ff), bf16),
            pltpu.VMEM((2, 2, CW, ff), bf16),
            pltpu.VMEM((2, ff, CW), bf16),
            pltpu.VMEM((2, rows, CW), bf16),
            pltpu.VMEM((2, rows // experts, CW), bf16),
            pltpu.VMEM((2, rows // experts, CW), bf16),
            pltpu.VMEM((tok, hidden), bf16),
            pltpu.VMEM((rows, 1), f32),
            dma((chunks, 3, 3)), dma((chunks, 3, 3)), dma((chunks,)), dma((chunks,)), dma((chunks,)),
            dma((2, 2)), dma((2,)), dma, pltpu.SemaphoreType.REGULAR,
        ],
        compiler_params=pltpu.CompilerParams(collective_id=0, has_side_effects=True, vmem_limit_bytes=67043328),
    )(tokens, slot_row, slot_col, rank_row, rank_col, gate_row, w_gate, w_up, w_down)


def solution(mesh):
    ep_axes = tuple(mesh.axis_names)
    num_devices = math.prod(mesh.shape[axis_name] for axis_name in ep_axes)
    row_spec = P(ep_axes, None)
    w_spec = P(ep_axes, None, None)

    def local_layer(tokens, expert_ids, gate_weights, w_gate, w_up, w_down):
        tok_dev, hidden = tokens.shape
        top_k = expert_ids.shape[1]
        local_experts = w_gate.shape[0]
        capacity = tok_dev * top_k // num_devices
        rows = num_devices * capacity
        all_experts = jnp.arange(num_devices * local_experts)
        gate_dense = jnp.sum(jnp.where(expert_ids[:, :, None] == all_experts[None, None, :], gate_weights[:, :, None], 0.0), axis=1)
        gate_send = gate_dense.reshape(tok_dev, num_devices, local_experts).transpose(1, 2, 0)
        gates = lax.all_to_all(gate_send, ep_axes, 0, 0, tiled=True)
        hit = jnp.any(gates > 0.0, axis=1)
        slot = jnp.where(hit, jnp.cumsum(hit.astype(jnp.int32), axis=1) - 1, -1)
        place = slot[:, None, :] == jnp.arange(capacity)[None, :, None]
        gate_pack = jnp.sum(jnp.where(place[:, None], gates[:, :, None, :], 0.0), axis=3)
        gate_pack = gate_pack.transpose(1, 0, 2).reshape(local_experts, rows)
        chosen = gate_pack > 0.0
        rank = jnp.where(chosen, jnp.cumsum(chosen.astype(jnp.int32), axis=1) - 1, -1)
        return moe_call(tokens, slot, slot.reshape(-1, 1), rank, rank.T, gate_pack, w_gate, w_up, w_down)

    return jax.shard_map(local_layer, mesh=mesh, in_specs=(row_spec, row_spec, row_spec, w_spec, w_spec, w_spec), out_specs=row_spec, check_vma=False)
```

```python
import math
import jax
import jax.numpy as jnp
from jax import lax
from jax.experimental import pallas as pl
from jax.experimental.pallas import tpu as pltpu
from jax.sharding import PartitionSpec as P

MESH = pl.DeviceIdType.MESH
CW = 256
ROW_PARTS = ((0, 96), (96, 80), (176, 80))
ALL = slice(None)
GATHER_STEPS = (
    (("x", (0, 0, 0), (0, 0, 1)), ("y", (0, 0, ALL), (0, 1, ALL)), ("z", (0, ALL, ALL), (1, ALL, ALL))),
    (("y", (0, 0, 0), (0, 1, 0)), ("z", (0, ALL, 0), (1, ALL, 0)), ("x", (ALL, ALL, 0), (ALL, ALL, 1))),
    (("z", (0, 0, 0), (1, 0, 0)), ("x", (ALL, 0, 0), (ALL, 0, 1)), ("y", (ALL, 0, ALL), (ALL, 1, ALL))),
)
SCATTER_STEPS = tuple(tuple((link, dst, src) for link, src, dst in steps[::-1]) for steps in GATHER_STEPS)
LANDING = ((1, 0, ALL, ALL), (1, 1, 0, ALL), (1, 1, 1, 0))


def moe_kernel(x_hbm, slot_row, slot_col, rank_row, rank_col, gate_row, w1_hbm, w3_hbm, w2_hbm, out_ref,
               g_buf, acc, sel, dense, hid, w13, w2, pair, x_exp, part, x_res, gate_col,
               step_send, step_recv, core_send, core_recv, x_sem, w13_sem, w2_sem, res_sem, ready):
    zb, yb, ex = lax.axis_index("ez"), lax.axis_index("ey"), lax.axis_index("ex")
    xb, cb = ex // 2, ex % 2
    peers = {
        "x": (zb, yb, (1 - xb) * 2 + cb),
        "y": (zb, 1 - yb, ex),
        "z": (1 - zb, yb, ex),
        "core": (zb, yb, xb * 2 + 1 - cb),
    }
    tok = x_hbm.shape[0]
    hidden = x_hbm.shape[1]
    chunks = hidden // CW
    experts, _, ff = w1_hbm.shape
    sources = slot_row.shape[0]
    rows = rank_col.shape[0]
    cap = rows // sources
    per_expert = rows // experts

    def xor(a, b):
        return a + b - 2 * a * b

    def source_of(rel):
        return (xor(zb, rel // 4 % 2) * 8 + xor(yb, rel // 2 % 2) * 4 + xor(xb, rel % 2) * 2 + xor(cb, rel // 8))

    def gather_copy(c, part, step):
        r0, n = ROW_PARTS[part]
        link, src, dst = GATHER_STEPS[part][step]
        return pltpu.make_async_remote_copy(
            g_buf.at[(c, 0) + src + (pl.ds(r0, n),)], g_buf.at[(c, 0) + dst + (pl.ds(r0, n),)],
            step_send.at[c, part, step], step_recv.at[c, part, step], device_id=peers[link], device_id_type=MESH)

    def gather_core(c):
        return pltpu.make_async_remote_copy(g_buf.at[c, 0], g_buf.at[c, 1], core_send.at[c], core_recv.at[c],
                                            device_id=peers["core"], device_id_type=MESH)

    def scatter_core(k):
        return pltpu.make_async_remote_copy(dense.at[k % 2, 1], g_buf.at[k, 0], core_send.at[k], core_recv.at[k],
                                            device_id=peers["core"], device_id_type=MESH)

    def scatter_copy(k, part, step):
        r0, n = ROW_PARTS[part]
        link, src, _ = SCATTER_STEPS[part][step]
        return pltpu.make_async_remote_copy(
            g_buf.at[(k, 0) + src + (pl.ds(r0, n),)], g_buf.at[(k,) + LANDING[step] + (pl.ds(r0, n),)],
            step_send.at[k, part, step], step_recv.at[k, part, step], device_id=peers[link], device_id_type=MESH)

    def x_copy(c):
        cols = pl.ds(pl.multiple_of(c * CW, CW), CW)
        return pltpu.make_async_copy(x_hbm.at[:, cols], g_buf.at[c, 0, 0, 0, 0], x_sem.at[c])

    def w13_copies(c, e):
        b = e % 2
        k_rows = pl.ds(pl.multiple_of(c * CW, CW), CW)
        return (pltpu.make_async_copy(w1_hbm.at[e, k_rows], w13.at[b, 0], w13_sem.at[b, 0]),
                pltpu.make_async_copy(w3_hbm.at[e, k_rows], w13.at[b, 1], w13_sem.at[b, 1]))

    def w2_copy(k, e):
        cols = pl.ds(pl.multiple_of(k * CW, CW), CW)
        return pltpu.make_async_copy(w2_hbm.at[e, :, cols], w2.at[e], w2_sem.at[e])

    def each(parts, fn):
        for part in parts:
            fn(part)

    PARTS = range(len(ROW_PARTS))

    for c in range(chunks):
        x_copy(c).start()
    res_copy = pltpu.make_async_copy(x_hbm, x_res, res_sem)
    res_copy.start()
    for e in range(2):
        for copy in w13_copies(0, e):
            copy.start()
    for e in range(experts):
        w2_copy(0, e).start()
    barrier = pltpu.get_barrier_semaphore()
    for peer in peers.values():
        pl.semaphore_signal(barrier, inc=1, device_id=peer, device_id_type=MESH)
    pl.semaphore_wait(barrier, len(peers))

    @jax.named_scope("start_first")
    def start_first(c):
        x_copy(c).wait()
        each(PARTS, lambda p: gather_copy(c, p, 0).start())

    @jax.named_scope("advance")
    def advance(c, step):
        def one(p):
            gather_copy(c, p, step - 1).wait_recv()
            gather_copy(c, p, step).start()
        each(PARTS, one)

    @jax.named_scope("to_core")
    def to_core(c):
        each(PARTS, lambda p: gather_copy(c, p, 2).wait_recv())
        gather_core(c).start()

    @jax.named_scope("pack")
    def pack(c):
        @pl.loop(0, sources // 8)
        def _(q):
            for u in range(8):
                rel = q * 8 + u
                s = source_of(rel)
                iota = lax.broadcasted_iota(jnp.int32, (cap, tok), 0)
                one_hot = jnp.where(slot_row[pl.ds(s, 1), :] == iota, 1.0, 0.0).astype(jnp.bfloat16)
                block = g_buf[c, rel // 8, rel // 4 % 2, rel // 2 % 2, rel % 2]
                packed = jnp.dot(one_hot, block, preferred_element_type=jnp.float32)
                pair[0, pl.ds(pl.multiple_of(s * cap, cap), cap), :] = packed.astype(jnp.bfloat16)

    def pick(e):
        x_exp[e % 2] = jnp.dot(sel[e * per_expert:(e + 1) * per_expert, :], pair[0], preferred_element_type=jnp.float32).astype(jnp.bfloat16)

    @jax.named_scope("up_project")
    def up_project(c, e):
        for copy in w13_copies(c, e):
            copy.wait()
        erows = slice(e * per_expert, (e + 1) * per_expert)

        def products():
            for j in range(2):
                for n in range(0, ff, CW):
                    acc[j, erows, n:n + CW] += jnp.dot(x_exp[e % 2], w13[e % 2, j, :, n:n + CW], preferred_element_type=jnp.float32)

        if e + 1 < experts:
            products()
            pick(e + 1)
        else:
            @pl.loop(0, (c + chunks) // chunks)
            def _(_):
                products()
        nc, ne = (c, e + 2) if e + 2 < experts else (c + 1, e + 2 - experts)

        @pl.when(nc < chunks)
        def _():
            for copy in w13_copies(nc, ne):
                copy.start()

    @jax.named_scope("build_pick")
    def build_pick():
        tile = 128

        @pl.loop(0, rows // tile)
        def _(t):
            e = t * tile // per_expert
            iota = lax.broadcasted_iota(jnp.int32, (tile, rows), 0) + t * tile % per_expert
            mask = rank_row[pl.ds(e, 1), :] == iota
            trows = pl.ds(pl.multiple_of(t * tile, tile), tile)
            sel[trows, :] = jnp.where(mask, 1.0, 0.0).astype(jnp.bfloat16)
            gate_col[trows, :] = jnp.sum(jnp.where(mask, gate_row[pl.ds(e, 1), :], 0.0), axis=1, keepdims=True)

    @jax.named_scope("clear_sums")
    def clear_sums():
        @pl.loop(0, rows // 64)
        def _(t):
            trows = pl.ds(pl.multiple_of(t * 64, 64), 64)
            for j in range(2):
                acc[j, trows, :] = jnp.zeros((64, ff), jnp.float32)

    start_first(0)
    start_first(1)
    part[...] = jnp.zeros(part.shape, part.dtype)
    clear_sums()
    advance(0, 1)
    start_first(2)
    build_pick()
    advance(1, 1)
    advance(0, 2)
    start_first(3)
    advance(2, 1)
    advance(1, 2)
    to_core(0)

    @pl.loop(1, chunks + 1)
    def _(k):
        @pl.when(k + 3 < chunks)
        def _():
            start_first(k + 3)

        @pl.when(k + 2 < chunks)
        def _():
            advance(k + 2, 1)

        @pl.when(k + 1 < chunks)
        def _():
            advance(k + 1, 2)

        gather_core(k - 1).wait_recv()
        pack(k - 1)
        @pl.loop(0, (k - 1 + chunks) // chunks)
        def _(_):
            pick(0)

        for e in range(experts // 2):
            up_project(k - 1, e)

        @pl.when(k < chunks)
        def _():
            to_core(k)

        for e in range(experts // 2, experts):
            up_project(k - 1, e)

    @pl.loop(0, chunks)
    def _(c):
        for p in PARTS:
            for step in range(3):
                gather_copy(c, p, step).wait_send()
        gather_core(c).wait_send()

    for peer in peers.values():
        pl.semaphore_signal(ready, inc=1, device_id=peer, device_id_type=MESH)

    @pl.loop(0, rows // 128)
    def _(t):
        trows = pl.ds(pl.multiple_of(t * 128, 128), 128)
        hid[trows, :] = (jax.nn.silu(acc[0, trows, :]) * acc[1, trows, :]).astype(jnp.bfloat16)
        iota = lax.broadcasted_iota(jnp.int32, (128, per_expert), 1)
        for e in range(experts):
            mask = rank_col[trows, e:e + 1] == iota
            sel[trows, e * per_expert:(e + 1) * per_expert] = jnp.where(mask, 1.0, 0.0).astype(jnp.bfloat16)

    res_copy.wait()
    pl.semaphore_wait(ready, len(peers))

    def add_into(dst, others):
        total = dst[...].astype(jnp.float32)
        for other in others:
            total = total + other[...].astype(jnp.float32)
        dst[...] = total.astype(jnp.bfloat16)

    @jax.named_scope("sum_core")
    def sum_core(k):
        scatter_core(k).wait_recv()

        @pl.loop(0, 8)
        def _(j):
            idx = (j // 4, j // 2 % 2, j % 2)
            add_into(g_buf.at[(k, 0) + idx], [dense.at[(k % 2, 0) + idx]])

    @jax.named_scope("sum_first")
    def sum_first(k):
        for p in PARTS:
            scatter_copy(k, p, 0).wait_recv()
            r0, n = ROW_PARTS[p]
            add_into(g_buf.at[(k, 0) + SCATTER_STEPS[p][0][2] + (pl.ds(r0, n),)], [g_buf.at[(k,) + LANDING[0] + (pl.ds(r0, n),)]])

    @jax.named_scope("sum_second")
    def sum_second(k):
        for p in PARTS:
            scatter_copy(k, p, 1).wait_recv()
            r0, n = ROW_PARTS[p]
            add_into(g_buf.at[(k, 0) + SCATTER_STEPS[p][2][1] + (pl.ds(r0, n),)], [g_buf.at[k, 1, 1, 0, 1, pl.ds(r0, n)]])

    @jax.named_scope("finish")
    def finish(k):
        for p in PARTS:
            scatter_copy(k, p, 2).wait_recv()
        cols = pl.ds(pl.multiple_of(k * CW, CW), CW)
        moe = g_buf[k, 0, 0, 0, 0].astype(jnp.float32) + g_buf[k, 1, 1, 0, 0].astype(jnp.float32) + g_buf[k, 1, 1, 1, 0].astype(jnp.float32)
        out_ref[:, cols] = (x_res[:, cols].astype(jnp.float32) + moe).astype(jnp.bfloat16)

    def start_scatter(k):
        each(PARTS, lambda p: scatter_copy(k, p, 0).start())

    @jax.named_scope("down_project")
    def down_project(k):
        @pl.loop(0, experts // 2)
        def _(half):
            both = (half * 2, half * 2 + 1)
            for e in both:
                w2_copy(k, e).wait()
            for u, e in enumerate(both):
                erows = pl.ds(pl.multiple_of(e * per_expert, per_expert), per_expert)
                o = jnp.dot(hid[erows, :], w2[e], preferred_element_type=jnp.float32) * gate_col[erows, :]
                hi = o.astype(jnp.bfloat16)
                pair[0, erows, :] = hi
                pair[1, erows, :] = (o - hi.astype(jnp.float32)).astype(jnp.bfloat16)

            @pl.when(k + 1 < chunks)
            def _():
                for e in both:
                    w2_copy(k + 1, e).start()

    @jax.named_scope("combine")
    def combine(k):
        def spread(m):
            for core in range(2):
                s = m * 2 + core
                slots = slot_col[pl.ds(pl.multiple_of(s * tok, tok), tok), :]
                place = jnp.where(slots == lax.broadcasted_iota(jnp.int32, (tok, cap), 1), 1.0, 0.0).astype(jnp.bfloat16)
                block = jnp.dot(place, part[m % 2, core * cap:(core + 1) * cap, :], preferred_element_type=jnp.float32)
                dense[k % 2, xor(core, cb), xor(m // 4, zb), xor(m // 2 % 2, yb), xor(m % 2, xb)] = block.astype(jnp.bfloat16)

        chips = sources // 2

        @pl.loop(0, chips)
        def _(m):
            spread((m + chips - 1) % chips)
            chosen = sel[pl.ds(pl.multiple_of(m * 2 * cap, 2 * cap), 2 * cap), :]
            total = jnp.dot(chosen, pair[0], preferred_element_type=jnp.float32)
            total = total + jnp.dot(chosen, pair[1], preferred_element_type=jnp.float32)
            part[m % 2] = total.astype(jnp.bfloat16)

            @pl.when((m == 0) & (k >= 1))
            def _():
                start_scatter(k - 1)

        spread(chips - 1)

    @pl.loop(0, chunks + 4)
    def _(k):
        @pl.when((k >= 2) & (k <= chunks + 1))
        def _():
            sum_first(k - 2)

        @pl.when((k >= 3) & (k <= chunks + 2))
        def _():
            sum_second(k - 3)

        @pl.when((k >= 2) & (k <= chunks + 1))
        def _():
            each(PARTS, lambda p: scatter_copy(k - 2, p, 1).start())

        @pl.when((k >= 3) & (k <= chunks + 2))
        def _():
            each(PARTS, lambda p: scatter_copy(k - 3, p, 2).start())

        @pl.when(k < chunks)
        def _():
            down_project(k)

        @pl.when((k >= 1) & (k <= chunks))
        def _():
            sum_core(k - 1)

        @pl.when(k == chunks)
        def _():
            start_scatter(k - 1)

        @pl.when(k < chunks)
        def _():
            @pl.when(k >= 2)
            def _():
                scatter_core(k - 2).wait_send()

            combine(k)
            scatter_core(k).start()

        @pl.when(k >= 4)
        def _():
            finish(k - 4)

    for k in (chunks - 2, chunks - 1):
        scatter_core(k).wait_send()

    @pl.loop(0, chunks)
    def _(k):
        for p in PARTS:
            for step in range(3):
                scatter_copy(k, p, step).wait_send()


def moe_call(tokens, slot_row, slot_col, rank_row, rank_col, gate_row, w_gate, w_up, w_down):
    tok, hidden = tokens.shape
    experts, _, ff = w_gate.shape
    rows = rank_col.shape[0]
    chunks = hidden // CW
    bf16, f32 = jnp.bfloat16, jnp.float32
    vmem = pl.BlockSpec(memory_space=pltpu.VMEM)
    hbm = pl.BlockSpec(memory_space=pl.ANY)
    dma = pltpu.SemaphoreType.DMA
    return pl.pallas_call(
        moe_kernel,
        out_shape=jax.ShapeDtypeStruct((tok, hidden), bf16),
        in_specs=[hbm, vmem, vmem, vmem, vmem, vmem, hbm, hbm, hbm],
        out_specs=vmem,
        scratch_shapes=[
            pltpu.VMEM((chunks, 2, 2, 2, 2, tok, CW), bf16),
            pltpu.VMEM((2, rows, ff), f32),
            pltpu.VMEM((rows, rows), bf16),
            pltpu.VMEM((2, 2, 2, 2, 2, tok, CW), bf16),
            pltpu.VMEM((rows, ff), bf16),
            pltpu.VMEM((2, 2, CW, ff), bf16),
            pltpu.VMEM((experts, ff, CW), bf16),
            pltpu.VMEM((2, rows, CW), bf16),
            pltpu.VMEM((2, rows // experts, CW), bf16),
            pltpu.VMEM((2, 2 * rows // 16, CW), bf16),
            pltpu.VMEM((tok, hidden), bf16),
            pltpu.VMEM((rows, 1), f32),
            dma((chunks, 3, 3)), dma((chunks, 3, 3)), dma((chunks,)), dma((chunks,)), dma((chunks,)),
            dma((2, 2)), dma((experts,)), dma, pltpu.SemaphoreType.REGULAR,
        ],
        compiler_params=pltpu.CompilerParams(collective_id=0, has_side_effects=True, vmem_limit_bytes=67043328),
    )(tokens, slot_row, slot_col, rank_row, rank_col, gate_row, w_gate, w_up, w_down)


def solution(mesh):
    ep_axes = tuple(mesh.axis_names)
    num_devices = math.prod(mesh.shape[axis_name] for axis_name in ep_axes)
    row_spec = P(ep_axes, None)
    w_spec = P(ep_axes, None, None)

    def local_layer(tokens, expert_ids, gate_weights, w_gate, w_up, w_down):
        tok_dev, hidden = tokens.shape
        top_k = expert_ids.shape[1]
        local_experts = w_gate.shape[0]
        capacity = tok_dev * top_k // num_devices
        rows = num_devices * capacity
        all_experts = jnp.arange(num_devices * local_experts)
        gate_dense = jnp.sum(jnp.where(expert_ids[:, :, None] == all_experts[None, None, :], gate_weights[:, :, None], 0.0), axis=1)
        gate_send = gate_dense.reshape(tok_dev, num_devices, local_experts).transpose(1, 2, 0)
        gates = lax.all_to_all(gate_send, ep_axes, 0, 0, tiled=True)
        hit = jnp.any(gates > 0.0, axis=1)
        slot = jnp.where(hit, jnp.cumsum(hit.astype(jnp.int32), axis=1) - 1, -1)
        place = slot[:, None, :] == jnp.arange(capacity)[None, :, None]
        gate_pack = jnp.sum(jnp.where(place[:, None], gates[:, :, None, :], 0.0), axis=3)
        gate_pack = gate_pack.transpose(1, 0, 2).reshape(local_experts, rows)
        chosen = gate_pack > 0.0
        rank = jnp.where(chosen, jnp.cumsum(chosen.astype(jnp.int32), axis=1) - 1, -1)
        return moe_call(tokens, slot, slot.reshape(-1, 1), rank, rank.T, gate_pack, w_gate, w_up, w_down)

    return jax.shard_map(local_layer, mesh=mesh, in_specs=(row_spec, row_spec, row_spec, w_spec, w_spec, w_spec), out_specs=row_spec, check_vma=False)
```

```python
import math
import jax
import jax.numpy as jnp
from jax import lax
from jax.experimental import pallas as pl
from jax.experimental.pallas import tpu as pltpu
from jax.sharding import PartitionSpec as P

MESH = pl.DeviceIdType.MESH
CW = 256
ROW_PARTS = ((0, 96), (96, 80), (176, 80))
ALL = slice(None)
GATHER_STEPS = (
    (("x", (0, 0, 0), (0, 0, 1)), ("y", (0, 0, ALL), (0, 1, ALL)), ("z", (0, ALL, ALL), (1, ALL, ALL))),
    (("y", (0, 0, 0), (0, 1, 0)), ("z", (0, ALL, 0), (1, ALL, 0)), ("x", (ALL, ALL, 0), (ALL, ALL, 1))),
    (("z", (0, 0, 0), (1, 0, 0)), ("x", (ALL, 0, 0), (ALL, 0, 1)), ("y", (ALL, 0, ALL), (ALL, 1, ALL))),
)
SCATTER_STEPS = tuple(tuple((link, dst, src) for link, src, dst in steps[::-1]) for steps in GATHER_STEPS)
LANDING = ((1, 0, ALL, ALL), (1, 1, 0, ALL), (1, 1, 1, 0))


def moe_kernel(ids_ref, gates_ref, x_hbm, w1_hbm, w3_hbm, w2_hbm, out_ref,
               g_buf, acc, sel, dense, hid, w13, w2, pair, x_exp, part, x_res, gate_col,
               gate_send, gate_recv, pieces, slot_row, slot_col, rank_row, rank_col, pack_gate,
               step_send, step_recv, core_send, core_recv, x_sem, w13_sem, w2_sem, res_sem, gate_out, gate_in, ready):
    zb, yb, ex = lax.axis_index("ez"), lax.axis_index("ey"), lax.axis_index("ex")
    xb, cb = ex // 2, ex % 2
    peers = {
        "x": (zb, yb, (1 - xb) * 2 + cb),
        "y": (zb, 1 - yb, ex),
        "z": (1 - zb, yb, ex),
        "core": (zb, yb, xb * 2 + 1 - cb),
    }
    tok = x_hbm.shape[0]
    hidden = x_hbm.shape[1]
    chunks = hidden // CW
    experts, _, ff = w1_hbm.shape
    sources = slot_row.shape[0]
    rows = sel.shape[0]
    cap = rows // sources
    per_expert = rows // experts

    def xor(a, b):
        return a + b - 2 * a * b

    def source_of(rel):
        return (xor(zb, rel // 4 % 2) * 8 + xor(yb, rel // 2 % 2) * 4 + xor(xb, rel % 2) * 2 + xor(cb, rel // 8))

    me = zb * 8 + yb * 4 + ex

    def gate_copy(rel):
        target = (xor(zb, rel // 4 % 2), xor(yb, rel // 2 % 2), xor(xb, rel % 2) * 2 + xor(cb, rel // 8))
        return pltpu.make_async_remote_copy(gate_send.at[source_of(rel)], gate_recv.at[me], gate_out.at[rel], gate_in.at[rel],
                                            device_id=target, device_id_type=MESH)

    def gather_copy(c, part, step):
        r0, n = ROW_PARTS[part]
        link, src, dst = GATHER_STEPS[part][step]
        return pltpu.make_async_remote_copy(
            g_buf.at[(c, 0) + src + (pl.ds(r0, n),)], g_buf.at[(c, 0) + dst + (pl.ds(r0, n),)],
            step_send.at[c, part, step], step_recv.at[c, part, step], device_id=peers[link], device_id_type=MESH)

    def gather_core(c):
        return pltpu.make_async_remote_copy(g_buf.at[c, 0], g_buf.at[c, 1], core_send.at[c], core_recv.at[c],
                                            device_id=peers["core"], device_id_type=MESH)

    def scatter_core(k):
        return pltpu.make_async_remote_copy(dense.at[k % 2, 1], g_buf.at[k, 0], core_send.at[k], core_recv.at[k],
                                            device_id=peers["core"], device_id_type=MESH)

    def scatter_copy(k, part, step):
        r0, n = ROW_PARTS[part]
        link, src, _ = SCATTER_STEPS[part][step]
        return pltpu.make_async_remote_copy(
            g_buf.at[(k, 0) + src + (pl.ds(r0, n),)], g_buf.at[(k,) + LANDING[step] + (pl.ds(r0, n),)],
            step_send.at[k, part, step], step_recv.at[k, part, step], device_id=peers[link], device_id_type=MESH)

    def x_copy(c):
        cols = pl.ds(pl.multiple_of(c * CW, CW), CW)
        return pltpu.make_async_copy(x_hbm.at[:, cols], g_buf.at[c, 0, 0, 0, 0], x_sem.at[c])

    def w13_copies(c, e):
        b = e % 2
        k_rows = pl.ds(pl.multiple_of(c * CW, CW), CW)
        return (pltpu.make_async_copy(w1_hbm.at[e, k_rows], w13.at[b, 0], w13_sem.at[b, 0]),
                pltpu.make_async_copy(w3_hbm.at[e, k_rows], w13.at[b, 1], w13_sem.at[b, 1]))

    def w2_copy(k, e):
        cols = pl.ds(pl.multiple_of(k * CW, CW), CW)
        return pltpu.make_async_copy(w2_hbm.at[e, :, cols], w2.at[e], w2_sem.at[e])

    def each(parts, fn):
        for part in parts:
            fn(part)

    PARTS = range(len(ROW_PARTS))

    for c in range(chunks):
        x_copy(c).start()
    res_copy = pltpu.make_async_copy(x_hbm, x_res, res_sem)
    res_copy.start()
    for e in range(2):
        for copy in w13_copies(0, e):
            copy.start()
    for e in range(experts):
        w2_copy(0, e).start()
    barrier = pltpu.get_barrier_semaphore()
    for rel in range(1, sources):
        target = (xor(zb, rel // 4 % 2), xor(yb, rel // 2 % 2), xor(xb, rel % 2) * 2 + xor(cb, rel // 8))
        pl.semaphore_signal(barrier, inc=1, device_id=target, device_id_type=MESH)

    for d in range(sources):
        expert = lax.broadcasted_iota(jnp.int32, (experts, tok), 0) + d * experts
        total = jnp.zeros((experts, tok), jnp.float32)
        for j in range(ids_ref.shape[0]):
            total = total + jnp.where(ids_ref[j:j + 1, :] == expert, gates_ref[j:j + 1, :], 0.0)
        gate_send[d] = total
    gate_recv[me] = gate_send[me]
    pl.semaphore_wait(barrier, sources - 1)

    @jax.named_scope("start_first")
    def start_first(c):
        x_copy(c).wait()
        each(PARTS, lambda p: gather_copy(c, p, 0).start())

    @jax.named_scope("advance")
    def advance(c, step):
        def one(p):
            gather_copy(c, p, step - 1).wait_recv()
            gather_copy(c, p, step).start()
        each(PARTS, one)

    @jax.named_scope("to_core")
    def to_core(c):
        each(PARTS, lambda p: gather_copy(c, p, 2).wait_recv())
        gather_core(c).start()

    @jax.named_scope("pack")
    def pack(c):
        @pl.loop(0, sources // 8)
        def _(q):
            for u in range(8):
                rel = q * 8 + u
                s = source_of(rel)
                iota = lax.broadcasted_iota(jnp.int32, (cap, tok), 0)
                one_hot = jnp.where(slot_row[pl.ds(s, 1), :] == iota, 1.0, 0.0).astype(jnp.bfloat16)
                block = g_buf[c, rel // 8, rel // 4 % 2, rel // 2 % 2, rel % 2]
                packed = jnp.dot(one_hot, block, preferred_element_type=jnp.float32)
                pair[0, pl.ds(pl.multiple_of(s * cap, cap), cap), :] = packed.astype(jnp.bfloat16)

    def pick(e):
        x_exp[e % 2] = jnp.dot(sel[e * per_expert:(e + 1) * per_expert, :], pair[0], preferred_element_type=jnp.float32).astype(jnp.bfloat16)

    @jax.named_scope("up_project")
    def up_project(c, e):
        for copy in w13_copies(c, e):
            copy.wait()
        erows = slice(e * per_expert, (e + 1) * per_expert)

        def products():
            for j in range(2):
                for n in range(0, ff, CW):
                    acc[j, erows, n:n + CW] += jnp.dot(x_exp[e % 2], w13[e % 2, j, :, n:n + CW], preferred_element_type=jnp.float32)

        if e + 1 < experts:
            products()
            pick(e + 1)
        else:
            @pl.loop(0, (c + chunks) // chunks)
            def _(_):
                products()
        nc, ne = (c, e + 2) if e + 2 < experts else (c + 1, e + 2 - experts)

        @pl.when(nc < chunks)
        def _():
            for copy in w13_copies(nc, ne):
                copy.start()

    def ones_where(mask):
        return jnp.where(mask, 1.0, 0.0).astype(jnp.bfloat16)

    @jax.named_scope("build_tables")
    def build_tables():
        i32, f32, bf16 = jnp.int32, jnp.float32, jnp.bfloat16

        def prefix(n):
            return ones_where(lax.broadcasted_iota(i32, (n, n), 0) <= lax.broadcasted_iota(i32, (n, n), 1))

        for rel in range(1, sources):
            gate_copy(rel).wait_recv()
        best = gate_recv[:, 0, :]
        for e in range(1, experts):
            best = jnp.maximum(best, gate_recv[:, e, :])
        hit = best > 0.0
        count = jnp.dot(ones_where(hit), prefix(tok), preferred_element_type=f32)
        slots = jnp.where(hit, count - 1.0, -1.0)
        slot_row[...] = slots.astype(i32)
        slots_t = jnp.transpose(jnp.concatenate([slots, jnp.zeros((128 - sources, tok), f32)], axis=0)).astype(i32)
        for s in range(sources):
            slot_col[s * tok:(s + 1) * tok, :] = slots_t[:, s:s + 1]
        for s in range(sources):
            gs = gate_recv[s]
            hi = gs.astype(bf16).astype(f32)
            mid = (gs - hi).astype(bf16).astype(f32)
            pieces[s, 0:experts, :] = jnp.where(gs > 0.0, 1.0, 0.0)
            pieces[s, experts:2 * experts, :] = hi
            pieces[s, 2 * experts:3 * experts, :] = mid
            pieces[s, 3 * experts:4 * experts, :] = gs - hi - mid
        for s in range(sources):
            place = ones_where(slot_row[s:s + 1, :] == lax.broadcasted_iota(i32, (cap, tok), 0))
            packed = lax.dot_general(pieces[s].astype(bf16), place, (((1,), (1,)), ((), ())), preferred_element_type=f32)
            rank_row[s * experts:(s + 1) * experts, :] = packed[0:experts].astype(i32)
            pack_gate[s * experts:(s + 1) * experts, :] = packed[experts:2 * experts] + packed[2 * experts:3 * experts] + packed[3 * experts:]
        n = sources * experts
        chosen = rank_row[...].astype(f32)
        count = jnp.dot(chosen.astype(bf16), prefix(cap), preferred_element_type=f32)
        r, c = lax.broadcasted_iota(i32, (n, n), 0), lax.broadcasted_iota(i32, (n, n), 1)
        earlier = ones_where(((r & (experts - 1)) == (c & (experts - 1))) & (c < r))
        before = jnp.sum(jnp.dot(earlier, chosen.astype(bf16), preferred_element_type=f32), axis=1, keepdims=True)
        rank = jnp.where(chosen > 0.0, count + before - 1.0, -1.0)
        rank_row[...] = rank.astype(i32)
        rank_t = jnp.transpose(jnp.concatenate([rank, jnp.zeros((128 - n, cap), f32)], axis=0)).astype(i32)
        for s in range(sources):
            rank_col[s * cap:(s + 1) * cap, :] = rank_t[:, s * experts:(s + 1) * experts]

    @jax.named_scope("build_pick")
    def build_pick():
        tile = 128

        @pl.loop(0, rows // tile)
        def _(t):
            e = t * tile // per_expert
            iota = lax.broadcasted_iota(jnp.int32, (tile, cap), 0) + t * tile % per_expert
            trows = pl.ds(pl.multiple_of(t * tile, tile), tile)
            gate = jnp.zeros((tile, cap), jnp.float32)
            for s in range(sources):
                mask = rank_row[pl.ds(s * experts + e, 1), :] == iota
                sel[trows, s * cap:(s + 1) * cap] = ones_where(mask)
                gate = gate + jnp.where(mask, pack_gate[pl.ds(s * experts + e, 1), :], 0.0)
            gate_col[trows, :] = jnp.sum(gate, axis=1, keepdims=True)

    @jax.named_scope("clear_sums")
    def clear_sums():
        @pl.loop(0, rows // 64)
        def _(t):
            trows = pl.ds(pl.multiple_of(t * 64, 64), 64)
            for j in range(2):
                acc[j, trows, :] = jnp.zeros((64, ff), jnp.float32)

    for rel in range(1, sources):
        gate_copy(rel).start()
    start_first(0)
    start_first(1)
    start_first(2)
    clear_sums()
    advance(0, 1)
    build_tables()
    advance(1, 1)
    advance(0, 2)
    build_pick()
    start_first(3)
    advance(2, 1)
    advance(1, 2)
    to_core(0)

    @pl.loop(1, chunks + 1)
    def _(k):
        @pl.when(k + 3 < chunks)
        def _():
            start_first(k + 3)

        @pl.when(k + 2 < chunks)
        def _():
            advance(k + 2, 1)

        @pl.when(k + 1 < chunks)
        def _():
            advance(k + 1, 2)

        gather_core(k - 1).wait_recv()
        pack(k - 1)
        @pl.loop(0, (k - 1 + chunks) // chunks)
        def _(_):
            pick(0)

        for e in range(experts // 2):
            up_project(k - 1, e)

        @pl.when(k < chunks)
        def _():
            to_core(k)

        for e in range(experts // 2, experts):
            up_project(k - 1, e)

    @pl.loop(0, chunks)
    def _(c):
        for p in PARTS:
            for step in range(3):
                gather_copy(c, p, step).wait_send()
        gather_core(c).wait_send()

    for rel in range(1, sources):
        gate_copy(rel).wait_send()
    for peer in peers.values():
        pl.semaphore_signal(ready, inc=1, device_id=peer, device_id_type=MESH)

    @pl.loop(0, rows // 128)
    def _(t):
        trows = pl.ds(pl.multiple_of(t * 128, 128), 128)
        hid[trows, :] = (jax.nn.silu(acc[0, trows, :]) * acc[1, trows, :]).astype(jnp.bfloat16)
        iota = lax.broadcasted_iota(jnp.int32, (128, per_expert), 1)
        for e in range(experts):
            mask = rank_col[trows, e:e + 1] == iota
            sel[trows, e * per_expert:(e + 1) * per_expert] = jnp.where(mask, 1.0, 0.0).astype(jnp.bfloat16)

    res_copy.wait()
    pl.semaphore_wait(ready, len(peers))

    def add_into(dst, others):
        total = dst[...].astype(jnp.float32)
        for other in others:
            total = total + other[...].astype(jnp.float32)
        dst[...] = total.astype(jnp.bfloat16)

    @jax.named_scope("sum_core")
    def sum_core(k):
        scatter_core(k).wait_recv()

        @pl.loop(0, 8)
        def _(j):
            idx = (j // 4, j // 2 % 2, j % 2)
            add_into(g_buf.at[(k, 0) + idx], [dense.at[(k % 2, 0) + idx]])

    @jax.named_scope("sum_first")
    def sum_first(k):
        for p in PARTS:
            scatter_copy(k, p, 0).wait_recv()
            r0, n = ROW_PARTS[p]
            add_into(g_buf.at[(k, 0) + SCATTER_STEPS[p][0][2] + (pl.ds(r0, n),)], [g_buf.at[(k,) + LANDING[0] + (pl.ds(r0, n),)]])

    @jax.named_scope("sum_second")
    def sum_second(k):
        for p in PARTS:
            scatter_copy(k, p, 1).wait_recv()
            r0, n = ROW_PARTS[p]
            add_into(g_buf.at[(k, 0) + SCATTER_STEPS[p][2][1] + (pl.ds(r0, n),)], [g_buf.at[k, 1, 1, 0, 1, pl.ds(r0, n)]])

    @jax.named_scope("finish")
    def finish(k):
        for p in PARTS:
            scatter_copy(k, p, 2).wait_recv()
        cols = pl.ds(pl.multiple_of(k * CW, CW), CW)
        moe = g_buf[k, 0, 0, 0, 0].astype(jnp.float32) + g_buf[k, 1, 1, 0, 0].astype(jnp.float32) + g_buf[k, 1, 1, 1, 0].astype(jnp.float32)
        out_ref[:, cols] = (x_res[:, cols].astype(jnp.float32) + moe).astype(jnp.bfloat16)

    def start_scatter(k):
        each(PARTS, lambda p: scatter_copy(k, p, 0).start())

    @jax.named_scope("down_project")
    def down_project(k):
        @pl.loop(0, experts // 2)
        def _(half):
            both = (half * 2, half * 2 + 1)
            for e in both:
                w2_copy(k, e).wait()
            for u, e in enumerate(both):
                erows = pl.ds(pl.multiple_of(e * per_expert, per_expert), per_expert)
                o = jnp.dot(hid[erows, :], w2[e], preferred_element_type=jnp.float32) * gate_col[erows, :]
                hi = o.astype(jnp.bfloat16)
                pair[0, erows, :] = hi
                pair[1, erows, :] = (o - hi.astype(jnp.float32)).astype(jnp.bfloat16)

            @pl.when(k + 1 < chunks)
            def _():
                for e in both:
                    w2_copy(k + 1, e).start()

    @jax.named_scope("combine")
    def combine(k):
        def spread(m):
            for core in range(2):
                s = m * 2 + core
                slots = slot_col[s * tok:(s + 1) * tok, :]
                place = jnp.where(slots == lax.broadcasted_iota(jnp.int32, (tok, cap), 1), 1.0, 0.0).astype(jnp.bfloat16)
                block = jnp.dot(place, part[m % 2, core * cap:(core + 1) * cap, :], preferred_element_type=jnp.float32)
                dense[k % 2, xor(core, cb), xor(m // 4, zb), xor(m // 2 % 2, yb), xor(m % 2, xb)] = block.astype(jnp.bfloat16)

        chips = sources // 2

        for m in range(chips + 1):
            if m:
                spread(m - 1)
            if m < chips:
                chosen = sel[m * 2 * cap:(m + 1) * 2 * cap, :]
                total = jnp.dot(chosen, pair[0], preferred_element_type=jnp.float32)
                total = total + jnp.dot(chosen, pair[1], preferred_element_type=jnp.float32)
                part[m % 2] = total.astype(jnp.bfloat16)

    @pl.loop(0, chunks + 4)
    def _(k):
        @pl.when((k >= 2) & (k <= chunks + 1))
        def _():
            sum_first(k - 2)

        @pl.when((k >= 3) & (k <= chunks + 2))
        def _():
            sum_second(k - 3)

        @pl.when((k >= 2) & (k <= chunks + 1))
        def _():
            each(PARTS, lambda p: scatter_copy(k - 2, p, 1).start())

        @pl.when((k >= 3) & (k <= chunks + 2))
        def _():
            each(PARTS, lambda p: scatter_copy(k - 3, p, 2).start())

        @pl.when(k < chunks)
        def _():
            down_project(k)

        @pl.when((k >= 1) & (k <= chunks))
        def _():
            sum_core(k - 1)

        @pl.when((k >= 1) & (k <= chunks))
        def _():
            start_scatter(k - 1)

        @pl.when(k < chunks)
        def _():
            @pl.when(k >= 2)
            def _():
                scatter_core(k - 2).wait_send()

            combine(k)
            scatter_core(k).start()

        @pl.when(k >= 4)
        def _():
            finish(k - 4)

    for k in (chunks - 2, chunks - 1):
        scatter_core(k).wait_send()

    @pl.loop(0, chunks)
    def _(k):
        for p in PARTS:
            for step in range(3):
                scatter_copy(k, p, step).wait_send()


def moe_call(expert_ids, gate_weights, tokens, w_gate, w_up, w_down, devices):
    tok, hidden = tokens.shape
    experts, _, ff = w_gate.shape
    cap = tok * expert_ids.shape[0] // devices
    rows = devices * cap
    chunks = hidden // CW
    bf16, f32, i32 = jnp.bfloat16, jnp.float32, jnp.int32
    vmem = pl.BlockSpec(memory_space=pltpu.VMEM)
    hbm = pl.BlockSpec(memory_space=pl.ANY)
    dma = pltpu.SemaphoreType.DMA
    return pl.pallas_call(
        moe_kernel,
        out_shape=jax.ShapeDtypeStruct((tok, hidden), bf16),
        in_specs=[vmem, vmem, hbm, hbm, hbm, hbm],
        out_specs=vmem,
        scratch_shapes=[
            pltpu.VMEM((chunks, 2, 2, 2, 2, tok, CW), bf16),
            pltpu.VMEM((2, rows, ff), f32),
            pltpu.VMEM((rows, rows), bf16),
            pltpu.VMEM((2, 2, 2, 2, 2, tok, CW), bf16),
            pltpu.VMEM((rows, ff), bf16),
            pltpu.VMEM((2, 2, CW, ff), bf16),
            pltpu.VMEM((experts, ff, CW), bf16),
            pltpu.VMEM((2, rows, CW), bf16),
            pltpu.VMEM((2, rows // experts, CW), bf16),
            pltpu.VMEM((2, 2 * cap, CW), bf16),
            pltpu.VMEM((tok, hidden), bf16),
            pltpu.VMEM((rows, 1), f32),
            pltpu.VMEM((devices, experts, tok), f32),
            pltpu.VMEM((devices, experts, tok), f32),
            pltpu.VMEM((devices, 4 * experts, tok), f32),
            pltpu.VMEM((devices, tok), i32),
            pltpu.VMEM((devices * tok, 1), i32),
            pltpu.VMEM((devices * experts, cap), i32),
            pltpu.VMEM((rows, experts), i32),
            pltpu.VMEM((devices * experts, cap), f32),
            dma((chunks, 3, 3)), dma((chunks, 3, 3)), dma((chunks,)), dma((chunks,)), dma((chunks,)),
            dma((2, 2)), dma((experts,)), dma, dma((devices,)), dma((devices,)), pltpu.SemaphoreType.REGULAR,
        ],
        compiler_params=pltpu.CompilerParams(collective_id=0, has_side_effects=True, vmem_limit_bytes=67043328),
    )(expert_ids, gate_weights, tokens, w_gate, w_up, w_down)


def solution(mesh):
    ep_axes = tuple(mesh.axis_names)
    num_devices = math.prod(mesh.shape[axis_name] for axis_name in ep_axes)
    row_spec = P(ep_axes, None)
    w_spec = P(ep_axes, None, None)

    def local_layer(tokens, expert_ids, gate_weights, w_gate, w_up, w_down):
        return moe_call(expert_ids.T, gate_weights.T, tokens, w_gate, w_up, w_down, num_devices)

    return jax.shard_map(local_layer, mesh=mesh, in_specs=(row_spec, row_spec, row_spec, w_spec, w_spec, w_spec), out_specs=row_spec, check_vma=False)
```

```python
import math
import jax
import jax.numpy as jnp
from jax import lax
from jax.experimental import pallas as pl
from jax.experimental.pallas import tpu as pltpu
from jax.sharding import PartitionSpec as P

MESH = pl.DeviceIdType.MESH
CW = 256
ROW_PARTS = ((0, 96), (96, 80), (176, 80))
ALL = slice(None)
GATHER_STEPS = (
    (("x", (0, 0, 0), (0, 0, 1)), ("y", (0, 0, ALL), (0, 1, ALL)), ("z", (0, ALL, ALL), (1, ALL, ALL))),
    (("y", (0, 0, 0), (0, 1, 0)), ("z", (0, ALL, 0), (1, ALL, 0)), ("x", (ALL, ALL, 0), (ALL, ALL, 1))),
    (("z", (0, 0, 0), (1, 0, 0)), ("x", (ALL, 0, 0), (ALL, 0, 1)), ("y", (ALL, 0, ALL), (ALL, 1, ALL))),
)
SCATTER_STEPS = tuple(tuple((link, dst, src) for link, src, dst in steps[::-1]) for steps in GATHER_STEPS)
LANDING = ((1, 0, ALL, ALL), (1, 1, 0, ALL), (1, 1, 1, 0))


def moe_kernel(ids_ref, gates_ref, x_hbm, w1_hbm, w3_hbm, w2_hbm, out_ref,
               g_buf, acc, sel, dense, hid, w13, w2, pair, x_exp, part, x_res, gate_col,
               gate_send, gate_recv, pieces, slot_row, slot_col, rank_row, rank_col, pack_gate,
               step_send, step_recv, core_send, core_recv, x_sem, w13_sem, w2_sem, res_sem, gate_out, gate_in, ready):
    zb, yb, ex = lax.axis_index("ez"), lax.axis_index("ey"), lax.axis_index("ex")
    xb, cb = ex // 2, ex % 2
    peers = {
        "x": (zb, yb, (1 - xb) * 2 + cb),
        "y": (zb, 1 - yb, ex),
        "z": (1 - zb, yb, ex),
        "core": (zb, yb, xb * 2 + 1 - cb),
    }
    tok = x_hbm.shape[0]
    hidden = x_hbm.shape[1]
    chunks = hidden // CW
    experts, _, ff = w1_hbm.shape
    sources = slot_row.shape[0]
    rows = sel.shape[0]
    cap = rows // sources
    per_expert = rows // experts

    def xor(a, b):
        return a + b - 2 * a * b

    def source_of(rel):
        return (xor(zb, rel // 4 % 2) * 8 + xor(yb, rel // 2 % 2) * 4 + xor(xb, rel % 2) * 2 + xor(cb, rel // 8))

    me = zb * 8 + yb * 4 + ex

    def gate_copy(rel):
        target = (xor(zb, rel // 4 % 2), xor(yb, rel // 2 % 2), xor(xb, rel % 2) * 2 + xor(cb, rel // 8))
        return pltpu.make_async_remote_copy(gate_send.at[source_of(rel)], gate_recv.at[me], gate_out.at[rel], gate_in.at[rel],
                                            device_id=target, device_id_type=MESH)

    def gather_copy(c, part, step):
        r0, n = ROW_PARTS[part]
        link, src, dst = GATHER_STEPS[part][step]
        return pltpu.make_async_remote_copy(
            g_buf.at[(c, 0) + src + (pl.ds(r0, n),)], g_buf.at[(c, 0) + dst + (pl.ds(r0, n),)],
            step_send.at[c, part, step], step_recv.at[c, part, step], device_id=peers[link], device_id_type=MESH)

    def gather_core(c):
        return pltpu.make_async_remote_copy(g_buf.at[c, 0], g_buf.at[c, 1], core_send.at[c], core_recv.at[c],
                                            device_id=peers["core"], device_id_type=MESH)

    def scatter_core(k):
        return pltpu.make_async_remote_copy(dense.at[k % 2, 1], g_buf.at[k, 0], core_send.at[k], core_recv.at[k],
                                            device_id=peers["core"], device_id_type=MESH)

    def scatter_copy(k, part, step):
        r0, n = ROW_PARTS[part]
        link, src, _ = SCATTER_STEPS[part][step]
        return pltpu.make_async_remote_copy(
            g_buf.at[(k, 0) + src + (pl.ds(r0, n),)], g_buf.at[(k,) + LANDING[step] + (pl.ds(r0, n),)],
            step_send.at[k, part, step], step_recv.at[k, part, step], device_id=peers[link], device_id_type=MESH)

    def x_copy(c):
        cols = pl.ds(pl.multiple_of(c * CW, CW), CW)
        return pltpu.make_async_copy(x_hbm.at[:, cols], g_buf.at[c, 0, 0, 0, 0], x_sem.at[c])

    def w13_copies(c, e):
        b = e % 2
        k_rows = pl.ds(pl.multiple_of(c * CW, CW), CW)
        return (pltpu.make_async_copy(w1_hbm.at[e, k_rows], w13.at[b, 0], w13_sem.at[b, 0]),
                pltpu.make_async_copy(w3_hbm.at[e, k_rows], w13.at[b, 1], w13_sem.at[b, 1]))

    def w2_copy(k, e):
        cols = pl.ds(pl.multiple_of(k * CW, CW), CW)
        return pltpu.make_async_copy(w2_hbm.at[e, :, cols], w2.at[e], w2_sem.at[e])

    def each(parts, fn):
        for part in parts:
            fn(part)

    PARTS = range(len(ROW_PARTS))

    barrier = pltpu.get_barrier_semaphore()
    for rel in range(1, sources):
        target = (xor(zb, rel // 4 % 2), xor(yb, rel // 2 % 2), xor(xb, rel % 2) * 2 + xor(cb, rel // 8))
        pl.semaphore_signal(barrier, inc=1, device_id=target, device_id_type=MESH)

    for c in range(chunks):
        x_copy(c).start()
    res_copy = pltpu.make_async_copy(x_hbm, x_res, res_sem)
    res_copy.start()
    for e in range(2):
        for copy in w13_copies(0, e):
            copy.start()
    for e in range(experts):
        w2_copy(0, e).start()
    for d in range(sources):
        expert = lax.broadcasted_iota(jnp.int32, (experts, tok), 0) + d * experts
        total = jnp.zeros((experts, tok), jnp.float32)
        for j in range(ids_ref.shape[0]):
            total = total + jnp.where(ids_ref[j:j + 1, :] == expert, gates_ref[j:j + 1, :], 0.0)
        gate_send[d] = total
    gate_recv[me] = gate_send[me]
    part[...] = jnp.zeros(part.shape, part.dtype)
    pl.semaphore_wait(barrier, sources - 1)

    @jax.named_scope("start_first")
    def start_first(c):
        x_copy(c).wait()
        each(PARTS, lambda p: gather_copy(c, p, 0).start())

    @jax.named_scope("advance")
    def advance(c, step):
        def one(p):
            gather_copy(c, p, step - 1).wait_recv()
            gather_copy(c, p, step).start()
        each(PARTS, one)

    @jax.named_scope("to_core")
    def to_core(c):
        each(PARTS, lambda p: gather_copy(c, p, 2).wait_recv())
        gather_core(c).start()

    @jax.named_scope("pack")
    def pack(c):
        @pl.loop(0, sources // 8)
        def _(q):
            for u in range(8):
                rel = q * 8 + u
                s = source_of(rel)
                iota = lax.broadcasted_iota(jnp.int32, (cap, tok), 0)
                one_hot = jnp.where(slot_row[pl.ds(s, 1), :] == iota, 1.0, 0.0).astype(jnp.bfloat16)
                block = g_buf[c, rel // 8, rel // 4 % 2, rel // 2 % 2, rel % 2]
                packed = jnp.dot(one_hot, block, preferred_element_type=jnp.float32)
                pair[0, pl.ds(pl.multiple_of(s * cap, cap), cap), :] = packed.astype(jnp.bfloat16)

    def pick(e):
        x_exp[e % 2] = jnp.dot(sel[e * per_expert:(e + 1) * per_expert, :], pair[0], preferred_element_type=jnp.float32).astype(jnp.bfloat16)

    @jax.named_scope("up_project")
    def up_project(c, e):
        for copy in w13_copies(c, e):
            copy.wait()
        erows = slice(e * per_expert, (e + 1) * per_expert)

        def products():
            for j in range(2):
                for n in range(0, ff, CW):
                    acc[j, erows, n:n + CW] += jnp.dot(x_exp[e % 2], w13[e % 2, j, :, n:n + CW], preferred_element_type=jnp.float32)

        if e + 1 < experts:
            products()
            pick(e + 1)
        else:
            @pl.loop(0, (c + chunks) // chunks)
            def _(_):
                products()
        nc, ne = (c, e + 2) if e + 2 < experts else (c + 1, e + 2 - experts)

        @pl.when(nc < chunks)
        def _():
            for copy in w13_copies(nc, ne):
                copy.start()

    def ones_where(mask):
        return jnp.where(mask, 1.0, 0.0).astype(jnp.bfloat16)

    @jax.named_scope("build_tables")
    def build_tables():
        i32, f32, bf16 = jnp.int32, jnp.float32, jnp.bfloat16

        def prefix(n):
            return ones_where(lax.broadcasted_iota(i32, (n, n), 0) <= lax.broadcasted_iota(i32, (n, n), 1))

        for rel in range(1, sources):
            gate_copy(rel).wait_recv()
        best = gate_recv[:, 0, :]
        for e in range(1, experts):
            best = jnp.maximum(best, gate_recv[:, e, :])
        hit = best > 0.0
        count = jnp.dot(ones_where(hit), prefix(tok), preferred_element_type=f32)
        slots = jnp.where(hit, count - 1.0, -1.0)
        slot_row[...] = slots.astype(i32)
        slots_t = jnp.transpose(jnp.concatenate([slots, jnp.zeros((128 - sources, tok), f32)], axis=0)).astype(i32)
        for s in range(sources):
            slot_col[s * tok:(s + 1) * tok, :] = slots_t[:, s:s + 1]
        for s in range(sources):
            gs = gate_recv[s]
            hi = gs.astype(bf16).astype(f32)
            mid = (gs - hi).astype(bf16).astype(f32)
            pieces[s, 0:experts, :] = jnp.where(gs > 0.0, 1.0, 0.0)
            pieces[s, experts:2 * experts, :] = hi
            pieces[s, 2 * experts:3 * experts, :] = mid
            pieces[s, 3 * experts:4 * experts, :] = gs - hi - mid
        for s in range(sources):
            place = ones_where(slot_row[s:s + 1, :] == lax.broadcasted_iota(i32, (cap, tok), 0))
            packed = lax.dot_general(pieces[s].astype(bf16), place, (((1,), (1,)), ((), ())), preferred_element_type=f32)
            rank_row[s * experts:(s + 1) * experts, :] = packed[0:experts].astype(i32)
            pack_gate[s * experts:(s + 1) * experts, :] = packed[experts:2 * experts] + packed[2 * experts:3 * experts] + packed[3 * experts:]
        n = sources * experts
        chosen = rank_row[...].astype(f32)
        count = jnp.dot(chosen.astype(bf16), prefix(cap), preferred_element_type=f32)
        r, c = lax.broadcasted_iota(i32, (n, n), 0), lax.broadcasted_iota(i32, (n, n), 1)
        earlier = ones_where(((r & (experts - 1)) == (c & (experts - 1))) & (c < r))
        before = jnp.sum(jnp.dot(earlier, chosen.astype(bf16), preferred_element_type=f32), axis=1, keepdims=True)
        rank = jnp.where(chosen > 0.0, count + before - 1.0, -1.0)
        rank_row[...] = rank.astype(i32)
        rank_t = jnp.transpose(jnp.concatenate([rank, jnp.zeros((128 - n, cap), f32)], axis=0)).astype(i32)
        for s in range(sources):
            rank_col[s * cap:(s + 1) * cap, :] = rank_t[:, s * experts:(s + 1) * experts]

    @jax.named_scope("build_pick")
    def build_pick():
        tile = 128

        @pl.loop(0, rows // tile)
        def _(t):
            e = t * tile // per_expert
            iota = lax.broadcasted_iota(jnp.int32, (tile, cap), 0) + t * tile % per_expert
            trows = pl.ds(pl.multiple_of(t * tile, tile), tile)
            gate = jnp.zeros((tile, cap), jnp.float32)
            for s in range(sources):
                mask = rank_row[pl.ds(s * experts + e, 1), :] == iota
                sel[trows, s * cap:(s + 1) * cap] = ones_where(mask)
                gate = gate + jnp.where(mask, pack_gate[pl.ds(s * experts + e, 1), :], 0.0)
            gate_col[trows, :] = jnp.sum(gate, axis=1, keepdims=True)

    @jax.named_scope("clear_sums")
    def clear_sums():
        @pl.loop(0, rows // 64)
        def _(t):
            trows = pl.ds(pl.multiple_of(t * 64, 64), 64)
            for j in range(2):
                acc[j, trows, :] = jnp.zeros((64, ff), jnp.float32)

    for rel in range(1, sources):
        gate_copy(rel).start()
    start_first(0)
    start_first(1)
    start_first(2)
    clear_sums()
    advance(0, 1)
    start_first(3)
    build_tables()
    advance(1, 1)
    advance(0, 2)
    build_pick()
    advance(2, 1)
    advance(1, 2)
    to_core(0)

    @pl.loop(1, chunks + 1)
    def _(k):
        @pl.when(k + 3 < chunks)
        def _():
            start_first(k + 3)

        @pl.when(k + 2 < chunks)
        def _():
            advance(k + 2, 1)

        @pl.when(k + 1 < chunks)
        def _():
            advance(k + 1, 2)

        gather_core(k - 1).wait_recv()
        pack(k - 1)
        @pl.loop(0, (k - 1 + chunks) // chunks)
        def _(_):
            pick(0)

        for e in range(experts // 2):
            up_project(k - 1, e)

        @pl.when(k < chunks)
        def _():
            to_core(k)

        for e in range(experts // 2, experts):
            up_project(k - 1, e)

    @pl.loop(0, chunks)
    def _(c):
        for p in PARTS:
            for step in range(3):
                gather_copy(c, p, step).wait_send()
        gather_core(c).wait_send()

    for rel in range(1, sources):
        gate_copy(rel).wait_send()
    for peer in peers.values():
        pl.semaphore_signal(ready, inc=1, device_id=peer, device_id_type=MESH)

    @pl.loop(0, rows // 128)
    def _(t):
        trows = pl.ds(pl.multiple_of(t * 128, 128), 128)
        hid[trows, :] = (jax.nn.silu(acc[0, trows, :]) * acc[1, trows, :]).astype(jnp.bfloat16)
        iota = lax.broadcasted_iota(jnp.int32, (128, per_expert), 1)
        for e in range(experts):
            mask = rank_col[trows, e:e + 1] == iota
            sel[trows, e * per_expert:(e + 1) * per_expert] = jnp.where(mask, 1.0, 0.0).astype(jnp.bfloat16)

    res_copy.wait()
    pl.semaphore_wait(ready, len(peers))

    def add_into(dst, others):
        total = dst[...].astype(jnp.float32)
        for other in others:
            total = total + other[...].astype(jnp.float32)
        dst[...] = total.astype(jnp.bfloat16)

    @jax.named_scope("sum_core")
    def sum_core(k):
        scatter_core(k).wait_recv()

        @pl.loop(0, 8)
        def _(j):
            idx = (j // 4, j // 2 % 2, j % 2)
            add_into(g_buf.at[(k, 0) + idx], [dense.at[(k % 2, 0) + idx]])

    @jax.named_scope("sum_first")
    def sum_first(k):
        for p in PARTS:
            scatter_copy(k, p, 0).wait_recv()
            r0, n = ROW_PARTS[p]
            add_into(g_buf.at[(k, 0) + SCATTER_STEPS[p][0][2] + (pl.ds(r0, n),)], [g_buf.at[(k,) + LANDING[0] + (pl.ds(r0, n),)]])

    @jax.named_scope("sum_second")
    def sum_second(k):
        for p in PARTS:
            scatter_copy(k, p, 1).wait_recv()
            r0, n = ROW_PARTS[p]
            add_into(g_buf.at[(k, 0) + SCATTER_STEPS[p][2][1] + (pl.ds(r0, n),)], [g_buf.at[k, 1, 1, 0, 1, pl.ds(r0, n)]])

    @jax.named_scope("finish")
    def finish(k):
        for p in PARTS:
            scatter_copy(k, p, 2).wait_recv()
        cols = pl.ds(pl.multiple_of(k * CW, CW), CW)
        moe = g_buf[k, 0, 0, 0, 0].astype(jnp.float32) + g_buf[k, 1, 1, 0, 0].astype(jnp.float32) + g_buf[k, 1, 1, 1, 0].astype(jnp.float32)
        out_ref[:, cols] = (x_res[:, cols].astype(jnp.float32) + moe).astype(jnp.bfloat16)

    def start_scatter(k):
        each(PARTS, lambda p: scatter_copy(k, p, 0).start())

    @jax.named_scope("down_project")
    def down_project(k):
        @pl.loop(0, experts // 2)
        def _(half):
            both = (half * 2, half * 2 + 1)
            for e in both:
                w2_copy(k, e).wait()
            for u, e in enumerate(both):
                erows = pl.ds(pl.multiple_of(e * per_expert, per_expert), per_expert)
                o = jnp.dot(hid[erows, :], w2[e], preferred_element_type=jnp.float32) * gate_col[erows, :]
                hi = o.astype(jnp.bfloat16)
                pair[0, erows, :] = hi
                pair[1, erows, :] = (o - hi.astype(jnp.float32)).astype(jnp.bfloat16)

            @pl.when(k + 1 < chunks)
            def _():
                for e in both:
                    w2_copy(k + 1, e).start()

    def combine(k):
        def spread(m):
            for core in range(2):
                s = m * 2 + core
                slots = slot_col[pl.ds(pl.multiple_of(s * tok, tok), tok), :] if not isinstance(s, int) else slot_col[s * tok:(s + 1) * tok, :]
                place = jnp.where(slots == lax.broadcasted_iota(jnp.int32, (tok, cap), 1), 1.0, 0.0).astype(jnp.bfloat16)
                block = jnp.dot(place, part[m % 2, core * cap:(core + 1) * cap, :], preferred_element_type=jnp.float32)
                dense[k % 2, xor(core, cb), xor(m // 4, zb), xor(m // 2 % 2, yb), xor(m % 2, xb)] = block.astype(jnp.bfloat16)

        chips = sources // 2

        def half(h):
            @pl.loop(h * chips // 2, (h + 1) * chips // 2)
            def _(m):
                spread((m + chips - 1) % chips)
                chosen = sel[pl.ds(pl.multiple_of(m * 2 * cap, 2 * cap), 2 * cap), :]
                total = jnp.dot(chosen, pair[0], preferred_element_type=jnp.float32)
                total = total + jnp.dot(chosen, pair[1], preferred_element_type=jnp.float32)
                part[m % 2] = total.astype(jnp.bfloat16)

        half(0)

        @pl.when(k >= 1)
        def _():
            sum_core(k - 1)
            start_scatter(k - 1)

        half(1)
        spread(chips - 1)

    @pl.loop(0, chunks + 4)
    def _(k):
        @pl.when((k >= 2) & (k <= chunks + 1))
        def _():
            sum_first(k - 2)

        @pl.when((k >= 3) & (k <= chunks + 2))
        def _():
            sum_second(k - 3)

        @pl.when((k >= 2) & (k <= chunks + 1))
        def _():
            each(PARTS, lambda p: scatter_copy(k - 2, p, 1).start())

        @pl.when((k >= 3) & (k <= chunks + 2))
        def _():
            each(PARTS, lambda p: scatter_copy(k - 3, p, 2).start())

        @pl.when(k < chunks)
        def _():
            down_project(k)

        @pl.when(k == chunks)
        def _():
            sum_core(k - 1)
            start_scatter(k - 1)

        @pl.when(k < chunks)
        def _():
            @pl.when(k >= 2)
            def _():
                scatter_core(k - 2).wait_send()

            combine(k)
            scatter_core(k).start()

        @pl.when(k >= 4)
        def _():
            finish(k - 4)

    for k in (chunks - 2, chunks - 1):
        scatter_core(k).wait_send()

    @pl.loop(0, chunks)
    def _(k):
        for p in PARTS:
            for step in range(3):
                scatter_copy(k, p, step).wait_send()


def moe_call(expert_ids, gate_weights, tokens, w_gate, w_up, w_down, devices):
    tok, hidden = tokens.shape
    experts, _, ff = w_gate.shape
    cap = tok * expert_ids.shape[0] // devices
    rows = devices * cap
    chunks = hidden // CW
    bf16, f32, i32 = jnp.bfloat16, jnp.float32, jnp.int32
    vmem = pl.BlockSpec(memory_space=pltpu.VMEM)
    hbm = pl.BlockSpec(memory_space=pl.ANY)
    dma = pltpu.SemaphoreType.DMA
    return pl.pallas_call(
        moe_kernel,
        out_shape=jax.ShapeDtypeStruct((tok, hidden), bf16),
        in_specs=[vmem, vmem, hbm, hbm, hbm, hbm],
        out_specs=vmem,
        scratch_shapes=[
            pltpu.VMEM((chunks, 2, 2, 2, 2, tok, CW), bf16),
            pltpu.VMEM((2, rows, ff), f32),
            pltpu.VMEM((rows, rows), bf16),
            pltpu.VMEM((2, 2, 2, 2, 2, tok, CW), bf16),
            pltpu.VMEM((rows, ff), bf16),
            pltpu.VMEM((2, 2, CW, ff), bf16),
            pltpu.VMEM((experts, ff, CW), bf16),
            pltpu.VMEM((2, rows, CW), bf16),
            pltpu.VMEM((2, rows // experts, CW), bf16),
            pltpu.VMEM((2, 2 * cap, CW), bf16),
            pltpu.VMEM((tok, hidden), bf16),
            pltpu.VMEM((rows, 1), f32),
            pltpu.VMEM((devices, experts, tok), f32),
            pltpu.VMEM((devices, experts, tok), f32),
            pltpu.VMEM((devices, 4 * experts, tok), f32),
            pltpu.VMEM((devices, tok), i32),
            pltpu.VMEM((devices * tok, 1), i32),
            pltpu.VMEM((devices * experts, cap), i32),
            pltpu.VMEM((rows, experts), i32),
            pltpu.VMEM((devices * experts, cap), f32),
            dma((chunks, 3, 3)), dma((chunks, 3, 3)), dma((chunks,)), dma((chunks,)), dma((chunks,)),
            dma((2, 2)), dma((experts,)), dma, dma((devices,)), dma((devices,)), pltpu.SemaphoreType.REGULAR,
        ],
        compiler_params=pltpu.CompilerParams(collective_id=0, has_side_effects=True, vmem_limit_bytes=67043328),
    )(expert_ids, gate_weights, tokens, w_gate, w_up, w_down)


def solution(mesh):
    ep_axes = tuple(mesh.axis_names)
    num_devices = math.prod(mesh.shape[axis_name] for axis_name in ep_axes)
    row_spec = P(ep_axes, None)
    w_spec = P(ep_axes, None, None)

    def local_layer(tokens, expert_ids, gate_weights, w_gate, w_up, w_down):
        return moe_call(expert_ids.T, gate_weights.T, tokens, w_gate, w_up, w_down, num_devices)

    return jax.shard_map(local_layer, mesh=mesh, in_specs=(row_spec, row_spec, row_spec, w_spec, w_spec, w_spec), out_specs=row_spec, check_vma=False)
```

```python
import math
import jax
import jax.numpy as jnp
from jax import lax
from jax.experimental import pallas as pl
from jax.experimental.pallas import tpu as pltpu
from jax.sharding import PartitionSpec as P

MESH = pl.DeviceIdType.MESH
CW = 256
ROW_PARTS = ((0, 96), (96, 80), (176, 80))
ALL = slice(None)
GATHER_STEPS = (
    (("x", (0, 0, 0), (0, 0, 1)), ("y", (0, 0, ALL), (0, 1, ALL)), ("z", (0, ALL, ALL), (1, ALL, ALL))),
    (("y", (0, 0, 0), (0, 1, 0)), ("z", (0, ALL, 0), (1, ALL, 0)), ("x", (ALL, ALL, 0), (ALL, ALL, 1))),
    (("z", (0, 0, 0), (1, 0, 0)), ("x", (ALL, 0, 0), (ALL, 0, 1)), ("y", (ALL, 0, ALL), (ALL, 1, ALL))),
)
SCATTER_STEPS = tuple(tuple((link, dst, src) for link, src, dst in steps[::-1]) for steps in GATHER_STEPS)
LANDING = ((1, 0, ALL, ALL), (1, 1, 0, ALL), (1, 1, 1, 0))


def moe_kernel(ids_ref, gates_ref, x_hbm, w1_hbm, w3_hbm, w2_hbm, out_ref,
               g_buf, acc, sel, dense, hid, w13, w2, pair, x_exp, part, x_res, gate_col,
               routes, gate_recv, pieces, slot_row, slot_col, rank_row, rank_col, pack_gate,
               step_send, step_recv, core_send, core_recv, x_sem, w13_sem, w2_sem, res_sem, route_send, route_recv, ready):
    zb, yb, ex = lax.axis_index("ez"), lax.axis_index("ey"), lax.axis_index("ex")
    xb, cb = ex // 2, ex % 2
    peers = {
        "x": (zb, yb, (1 - xb) * 2 + cb),
        "y": (zb, 1 - yb, ex),
        "z": (1 - zb, yb, ex),
        "core": (zb, yb, xb * 2 + 1 - cb),
    }
    tok = x_hbm.shape[0]
    hidden = x_hbm.shape[1]
    chunks = hidden // CW
    experts, _, ff = w1_hbm.shape
    sources = slot_row.shape[0]
    rows = sel.shape[0]
    cap = rows // sources
    per_expert = rows // experts

    def xor(a, b):
        return a + b - 2 * a * b

    def source_of(rel):
        return (xor(zb, rel // 4 % 2) * 8 + xor(yb, rel // 2 % 2) * 4 + xor(xb, rel % 2) * 2 + xor(cb, rel // 8))

    me = zb * 8 + yb * 4 + ex

    def table_copy(hop):
        src, dst = (((0, 0, 0, 0), (0, 0, 0, 1)), ((0, 0, 0), (0, 0, 1)), ((0, 0), (0, 1)), ((0,), (1,)))[hop]
        return pltpu.make_async_remote_copy(routes.at[src], routes.at[dst], route_send.at[hop], route_recv.at[hop],
                                            device_id=peers[("x", "y", "z", "core")[hop]], device_id_type=MESH)

    def gather_copy(c, part, step):
        r0, n = ROW_PARTS[part]
        link, src, dst = GATHER_STEPS[part][step]
        return pltpu.make_async_remote_copy(
            g_buf.at[(c, 0) + src + (pl.ds(r0, n),)], g_buf.at[(c, 0) + dst + (pl.ds(r0, n),)],
            step_send.at[c, part, step], step_recv.at[c, part, step], device_id=peers[link], device_id_type=MESH)

    def gather_core(c):
        return pltpu.make_async_remote_copy(g_buf.at[c, 0], g_buf.at[c, 1], core_send.at[c], core_recv.at[c],
                                            device_id=peers["core"], device_id_type=MESH)

    def scatter_core(k):
        return pltpu.make_async_remote_copy(dense.at[k % 2, 1], g_buf.at[k, 0], core_send.at[k], core_recv.at[k],
                                            device_id=peers["core"], device_id_type=MESH)

    def scatter_copy(k, part, step):
        r0, n = ROW_PARTS[part]
        link, src, _ = SCATTER_STEPS[part][step]
        return pltpu.make_async_remote_copy(
            g_buf.at[(k, 0) + src + (pl.ds(r0, n),)], g_buf.at[(k,) + LANDING[step] + (pl.ds(r0, n),)],
            step_send.at[k, part, step], step_recv.at[k, part, step], device_id=peers[link], device_id_type=MESH)

    def x_copy(c):
        cols = pl.ds(pl.multiple_of(c * CW, CW), CW)
        return pltpu.make_async_copy(x_hbm.at[:, cols], g_buf.at[c, 0, 0, 0, 0], x_sem.at[c])

    def w13_copies(c, e):
        b = e % 2
        k_rows = pl.ds(pl.multiple_of(c * CW, CW), CW)
        return (pltpu.make_async_copy(w1_hbm.at[e, k_rows], w13.at[b, 0], w13_sem.at[b, 0]),
                pltpu.make_async_copy(w3_hbm.at[e, k_rows], w13.at[b, 1], w13_sem.at[b, 1]))

    def w2_copy(k, e):
        cols = pl.ds(pl.multiple_of(k * CW, CW), CW)
        return pltpu.make_async_copy(w2_hbm.at[e, :, cols], w2.at[e], w2_sem.at[e])

    def each(parts, fn):
        for part in parts:
            fn(part)

    PARTS = range(len(ROW_PARTS))

    barrier = pltpu.get_barrier_semaphore()
    for peer in peers.values():
        pl.semaphore_signal(barrier, inc=1, device_id=peer, device_id_type=MESH)
    for c in range(chunks):
        x_copy(c).start()
    res_copy = pltpu.make_async_copy(x_hbm, x_res, res_sem)
    res_copy.start()
    for e in range(2):
        for copy in w13_copies(0, e):
            copy.start()
    for e in range(experts):
        w2_copy(0, e).start()
    top_k = ids_ref.shape[0]
    routes[0, 0, 0, 0, 0:top_k, :] = ids_ref[...].astype(jnp.float32)
    routes[0, 0, 0, 0, top_k:2 * top_k, :] = gates_ref[...]
    part[...] = jnp.zeros(part.shape, part.dtype)
    pl.semaphore_wait(barrier, len(peers))

    @jax.named_scope("start_first")
    def start_first(c):
        x_copy(c).wait()
        each(PARTS, lambda p: gather_copy(c, p, 0).start())

    @jax.named_scope("advance")
    def advance(c, step):
        def one(p):
            gather_copy(c, p, step - 1).wait_recv()
            gather_copy(c, p, step).start()
        each(PARTS, one)

    @jax.named_scope("to_core")
    def to_core(c):
        each(PARTS, lambda p: gather_copy(c, p, 2).wait_recv())
        gather_core(c).start()

    @jax.named_scope("pack")
    def pack(c):
        @pl.loop(0, sources // 8)
        def _(q):
            for u in range(8):
                rel = q * 8 + u
                s = source_of(rel)
                iota = lax.broadcasted_iota(jnp.int32, (cap, tok), 0)
                one_hot = jnp.where(slot_row[pl.ds(s, 1), :] == iota, 1.0, 0.0).astype(jnp.bfloat16)
                block = g_buf[c, rel // 8, rel // 4 % 2, rel // 2 % 2, rel % 2]
                packed = jnp.dot(one_hot, block, preferred_element_type=jnp.float32)
                pair[0, pl.ds(pl.multiple_of(s * cap, cap), cap), :] = packed.astype(jnp.bfloat16)

    def pick(e):
        x_exp[e % 2] = jnp.dot(sel[e * per_expert:(e + 1) * per_expert, :], pair[0], preferred_element_type=jnp.float32).astype(jnp.bfloat16)

    @jax.named_scope("up_project")
    def up_project(c, e):
        for copy in w13_copies(c, e):
            copy.wait()
        erows = slice(e * per_expert, (e + 1) * per_expert)

        def products():
            for j in range(2):
                for n in range(0, ff, CW):
                    acc[j, erows, n:n + CW] += jnp.dot(x_exp[e % 2], w13[e % 2, j, :, n:n + CW], preferred_element_type=jnp.float32)

        if e + 1 < experts:
            products()
            pick(e + 1)
        else:
            @pl.loop(0, (c + chunks) // chunks)
            def _(_):
                products()
        nc, ne = (c, e + 2) if e + 2 < experts else (c + 1, e + 2 - experts)

        @pl.when(nc < chunks)
        def _():
            for copy in w13_copies(nc, ne):
                copy.start()

    def ones_where(mask):
        return jnp.where(mask, 1.0, 0.0).astype(jnp.bfloat16)

    @jax.named_scope("build_tables")
    def build_tables():
        i32, f32, bf16 = jnp.int32, jnp.float32, jnp.bfloat16

        def prefix(n):
            return ones_where(lax.broadcasted_iota(i32, (n, n), 0) <= lax.broadcasted_iota(i32, (n, n), 1))

        for rel in range(sources):
            route = routes.at[rel // 8, rel // 4 % 2, rel // 2 % 2, rel % 2]
            expert = (lax.broadcasted_iota(i32, (experts, tok), 0) + me * experts).astype(f32)
            total = jnp.zeros((experts, tok), f32)
            for j in range(top_k):
                total = total + jnp.where(route[j:j + 1, :] == expert, route[top_k + j:top_k + j + 1, :], 0.0)
            gate_recv[source_of(rel)] = total
        best = gate_recv[:, 0, :]
        for e in range(1, experts):
            best = jnp.maximum(best, gate_recv[:, e, :])
        hit = best > 0.0
        count = jnp.dot(ones_where(hit), prefix(tok), preferred_element_type=f32)
        slots = jnp.where(hit, count - 1.0, -1.0)
        slot_row[...] = slots.astype(i32)
        slots_t = jnp.transpose(jnp.concatenate([slots, jnp.zeros((128 - sources, tok), f32)], axis=0)).astype(i32)
        for s in range(sources):
            slot_col[s * tok:(s + 1) * tok, :] = slots_t[:, s:s + 1]
        for s in range(sources):
            gs = gate_recv[s]
            hi = gs.astype(bf16).astype(f32)
            mid = (gs - hi).astype(bf16).astype(f32)
            pieces[s, 0:experts, :] = jnp.where(gs > 0.0, 1.0, 0.0)
            pieces[s, experts:2 * experts, :] = hi
            pieces[s, 2 * experts:3 * experts, :] = mid
            pieces[s, 3 * experts:4 * experts, :] = gs - hi - mid
        for s in range(sources):
            place = ones_where(slot_row[s:s + 1, :] == lax.broadcasted_iota(i32, (cap, tok), 0))
            packed = lax.dot_general(pieces[s].astype(bf16), place, (((1,), (1,)), ((), ())), preferred_element_type=f32)
            rank_row[s * experts:(s + 1) * experts, :] = packed[0:experts].astype(i32)
            pack_gate[s * experts:(s + 1) * experts, :] = packed[experts:2 * experts] + packed[2 * experts:3 * experts] + packed[3 * experts:]
        n = sources * experts
        chosen = rank_row[...].astype(f32)
        count = jnp.dot(chosen.astype(bf16), prefix(cap), preferred_element_type=f32)
        r, c = lax.broadcasted_iota(i32, (n, n), 0), lax.broadcasted_iota(i32, (n, n), 1)
        earlier = ones_where(((r & (experts - 1)) == (c & (experts - 1))) & (c < r))
        before = jnp.sum(jnp.dot(earlier, chosen.astype(bf16), preferred_element_type=f32), axis=1, keepdims=True)
        rank = jnp.where(chosen > 0.0, count + before - 1.0, -1.0)
        rank_row[...] = rank.astype(i32)
        rank_t = jnp.transpose(jnp.concatenate([rank, jnp.zeros((128 - n, cap), f32)], axis=0)).astype(i32)
        for s in range(sources):
            rank_col[s * cap:(s + 1) * cap, :] = rank_t[:, s * experts:(s + 1) * experts]

    @jax.named_scope("build_pick")
    def build_pick():
        tile = 128

        @pl.loop(0, rows // tile)
        def _(t):
            e = t * tile // per_expert
            iota = lax.broadcasted_iota(jnp.int32, (tile, cap), 0) + t * tile % per_expert
            trows = pl.ds(pl.multiple_of(t * tile, tile), tile)
            gate = jnp.zeros((tile, cap), jnp.float32)
            for s in range(sources):
                mask = rank_row[pl.ds(s * experts + e, 1), :] == iota
                sel[trows, s * cap:(s + 1) * cap] = ones_where(mask)
                gate = gate + jnp.where(mask, pack_gate[pl.ds(s * experts + e, 1), :], 0.0)
            gate_col[trows, :] = jnp.sum(gate, axis=1, keepdims=True)

    @jax.named_scope("clear_sums")
    def clear_sums():
        @pl.loop(0, rows // 64)
        def _(t):
            trows = pl.ds(pl.multiple_of(t * 64, 64), 64)
            for j in range(2):
                acc[j, trows, :] = jnp.zeros((64, ff), jnp.float32)

    def table_next(hop):
        table_copy(hop - 1).wait_recv()
        table_copy(hop).start()

    table_copy(0).start()
    start_first(0)
    start_first(1)
    clear_sums()
    table_next(1)
    advance(0, 1)
    start_first(2)
    table_next(2)
    advance(0, 2)
    advance(1, 1)
    table_next(3)
    start_first(3)
    table_copy(3).wait_recv()
    build_tables()
    advance(1, 2)
    advance(2, 1)
    build_pick()
    to_core(0)

    @pl.loop(1, chunks + 1)
    def _(k):
        @pl.when(k + 3 < chunks)
        def _():
            start_first(k + 3)

        @pl.when(k + 2 < chunks)
        def _():
            advance(k + 2, 1)

        @pl.when(k + 1 < chunks)
        def _():
            advance(k + 1, 2)

        gather_core(k - 1).wait_recv()
        pack(k - 1)
        @pl.loop(0, (k - 1 + chunks) // chunks)
        def _(_):
            pick(0)

        for e in range(experts // 2):
            up_project(k - 1, e)

        @pl.when(k < chunks)
        def _():
            to_core(k)

        for e in range(experts // 2, experts):
            up_project(k - 1, e)

    @pl.loop(0, chunks)
    def _(c):
        for p in PARTS:
            for step in range(3):
                gather_copy(c, p, step).wait_send()
        gather_core(c).wait_send()

    for hop in range(4):
        table_copy(hop).wait_send()
    for peer in peers.values():
        pl.semaphore_signal(ready, inc=1, device_id=peer, device_id_type=MESH)

    @pl.loop(0, rows // 128)
    def _(t):
        trows = pl.ds(pl.multiple_of(t * 128, 128), 128)
        hid[trows, :] = (jax.nn.silu(acc[0, trows, :]) * acc[1, trows, :]).astype(jnp.bfloat16)
        iota = lax.broadcasted_iota(jnp.int32, (128, per_expert), 1)
        for e in range(experts):
            mask = rank_col[trows, e:e + 1] == iota
            sel[trows, e * per_expert:(e + 1) * per_expert] = jnp.where(mask, 1.0, 0.0).astype(jnp.bfloat16)

    res_copy.wait()
    pl.semaphore_wait(ready, len(peers))

    def add_into(dst, others):
        total = dst[...].astype(jnp.float32)
        for other in others:
            total = total + other[...].astype(jnp.float32)
        dst[...] = total.astype(jnp.bfloat16)

    @jax.named_scope("sum_core")
    def sum_core(k):
        scatter_core(k).wait_recv()

        @pl.loop(0, 8)
        def _(j):
            idx = (j // 4, j // 2 % 2, j % 2)
            add_into(g_buf.at[(k, 0) + idx], [dense.at[(k % 2, 0) + idx]])

    @jax.named_scope("sum_first")
    def sum_first(k):
        for p in PARTS:
            scatter_copy(k, p, 0).wait_recv()
            r0, n = ROW_PARTS[p]
            add_into(g_buf.at[(k, 0) + SCATTER_STEPS[p][0][2] + (pl.ds(r0, n),)], [g_buf.at[(k,) + LANDING[0] + (pl.ds(r0, n),)]])

    @jax.named_scope("sum_second")
    def sum_second(k):
        for p in PARTS:
            scatter_copy(k, p, 1).wait_recv()
            r0, n = ROW_PARTS[p]
            add_into(g_buf.at[(k, 0) + SCATTER_STEPS[p][2][1] + (pl.ds(r0, n),)], [g_buf.at[k, 1, 1, 0, 1, pl.ds(r0, n)]])

    @jax.named_scope("finish")
    def finish(k):
        for p in PARTS:
            scatter_copy(k, p, 2).wait_recv()
        cols = pl.ds(pl.multiple_of(k * CW, CW), CW)
        moe = g_buf[k, 0, 0, 0, 0].astype(jnp.float32) + g_buf[k, 1, 1, 0, 0].astype(jnp.float32) + g_buf[k, 1, 1, 1, 0].astype(jnp.float32)
        out_ref[:, cols] = (x_res[:, cols].astype(jnp.float32) + moe).astype(jnp.bfloat16)

    def start_scatter(k):
        each(PARTS, lambda p: scatter_copy(k, p, 0).start())

    def reduce_step(k):
        @pl.when((k >= 1) & (k <= chunks))
        def _():
            sum_core(k - 1)

        @pl.when((k >= 1) & (k <= chunks))
        def _():
            start_scatter(k - 1)

        @pl.when((k >= 2) & (k <= chunks + 1))
        def _():
            sum_first(k - 2)
            each(PARTS, lambda p: scatter_copy(k - 2, p, 1).start())

        @pl.when((k >= 3) & (k <= chunks + 2))
        def _():
            sum_second(k - 3)
            each(PARTS, lambda p: scatter_copy(k - 3, p, 2).start())

        @pl.when(k >= 4)
        def _():
            finish(k - 4)

    @jax.named_scope("down_project")
    def down_project(k):
        @pl.loop(0, experts // 2)
        def _(half):
            both = (half * 2, half * 2 + 1)
            for e in both:
                w2_copy(k, e).wait()
            for u, e in enumerate(both):
                erows = pl.ds(pl.multiple_of(e * per_expert, per_expert), per_expert)
                o = jnp.dot(hid[erows, :], w2[e], preferred_element_type=jnp.float32) * gate_col[erows, :]
                hi = o.astype(jnp.bfloat16)
                pair[0, erows, :] = hi
                pair[1, erows, :] = (o - hi.astype(jnp.float32)).astype(jnp.bfloat16)

            @pl.when(k + 1 < chunks)
            def _():
                for e in both:
                    w2_copy(k + 1, e).start()

    def combine(k):
        def spread(m):
            for core in range(2):
                s = m * 2 + core
                slots = slot_col[pl.ds(pl.multiple_of(s * tok, tok), tok), :] if not isinstance(s, int) else slot_col[s * tok:(s + 1) * tok, :]
                place = jnp.where(slots == lax.broadcasted_iota(jnp.int32, (tok, cap), 1), 1.0, 0.0).astype(jnp.bfloat16)
                block = jnp.dot(place, part[m % 2, core * cap:(core + 1) * cap, :], preferred_element_type=jnp.float32)
                dense[k % 2, xor(core, cb), xor(m // 4, zb), xor(m // 2 % 2, yb), xor(m % 2, xb)] = block.astype(jnp.bfloat16)

        chips = sources // 2

        def half(h):
            @pl.loop(h * chips // 2, (h + 1) * chips // 2)
            def _(m):
                spread((m + chips - 1) % chips)
                chosen = sel[pl.ds(pl.multiple_of(m * 2 * cap, 2 * cap), 2 * cap), :]
                total = jnp.dot(chosen, pair[0], preferred_element_type=jnp.float32)
                total = total + jnp.dot(chosen, pair[1], preferred_element_type=jnp.float32)
                part[m % 2] = total.astype(jnp.bfloat16)

        half(0)
        reduce_step(k)
        half(1)
        spread(chips - 1)

    @pl.loop(0, chunks)
    def _(k):
        down_project(k)

        @pl.when(k >= 2)
        def _():
            scatter_core(k - 2).wait_send()

        combine(k)
        scatter_core(k).start()

    @pl.loop(chunks, chunks + 4)
    def _(k):
        reduce_step(k)

    for k in (chunks - 2, chunks - 1):
        scatter_core(k).wait_send()

    @pl.loop(0, chunks)
    def _(k):
        for p in PARTS:
            for step in range(3):
                scatter_copy(k, p, step).wait_send()


def moe_call(expert_ids, gate_weights, tokens, w_gate, w_up, w_down, devices):
    tok, hidden = tokens.shape
    experts, _, ff = w_gate.shape
    cap = tok * expert_ids.shape[0] // devices
    rows = devices * cap
    chunks = hidden // CW
    bf16, f32, i32 = jnp.bfloat16, jnp.float32, jnp.int32
    vmem = pl.BlockSpec(memory_space=pltpu.VMEM)
    hbm = pl.BlockSpec(memory_space=pl.ANY)
    dma = pltpu.SemaphoreType.DMA
    return pl.pallas_call(
        moe_kernel,
        out_shape=jax.ShapeDtypeStruct((tok, hidden), bf16),
        in_specs=[vmem, vmem, hbm, hbm, hbm, hbm],
        out_specs=vmem,
        scratch_shapes=[
            pltpu.VMEM((chunks, 2, 2, 2, 2, tok, CW), bf16),
            pltpu.VMEM((2, rows, ff), f32),
            pltpu.VMEM((rows, rows), bf16),
            pltpu.VMEM((2, 2, 2, 2, 2, tok, CW), bf16),
            pltpu.VMEM((rows, ff), bf16),
            pltpu.VMEM((2, 2, CW, ff), bf16),
            pltpu.VMEM((experts, ff, CW), bf16),
            pltpu.VMEM((2, rows, CW), bf16),
            pltpu.VMEM((2, rows // experts, CW), bf16),
            pltpu.VMEM((2, 2 * cap, CW), bf16),
            pltpu.VMEM((tok, hidden), bf16),
            pltpu.VMEM((rows, 1), f32),
            pltpu.VMEM((2, 2, 2, 2, 2 * expert_ids.shape[0], tok), f32),
            pltpu.VMEM((devices, experts, tok), f32),
            pltpu.VMEM((devices, 4 * experts, tok), f32),
            pltpu.VMEM((devices, tok), i32),
            pltpu.VMEM((devices * tok, 1), i32),
            pltpu.VMEM((devices * experts, cap), i32),
            pltpu.VMEM((rows, experts), i32),
            pltpu.VMEM((devices * experts, cap), f32),
            dma((chunks, 3, 3)), dma((chunks, 3, 3)), dma((chunks,)), dma((chunks,)), dma((chunks,)),
            dma((2, 2)), dma((experts,)), dma, dma((4,)), dma((4,)), pltpu.SemaphoreType.REGULAR,
        ],
        compiler_params=pltpu.CompilerParams(collective_id=0, has_side_effects=True, vmem_limit_bytes=67043328),
    )(expert_ids, gate_weights, tokens, w_gate, w_up, w_down)


def solution(mesh):
    ep_axes = tuple(mesh.axis_names)
    num_devices = math.prod(mesh.shape[axis_name] for axis_name in ep_axes)
    row_spec = P(ep_axes, None)
    w_spec = P(ep_axes, None, None)

    def local_layer(tokens, expert_ids, gate_weights, w_gate, w_up, w_down):
        return moe_call(expert_ids.T, gate_weights.T, tokens, w_gate, w_up, w_down, num_devices)

    return jax.shard_map(local_layer, mesh=mesh, in_specs=(row_spec, row_spec, row_spec, w_spec, w_spec, w_spec), out_specs=row_spec, check_vma=False)
```

```python
import math
import jax
import jax.numpy as jnp
from jax import lax
from jax.experimental import pallas as pl
from jax.experimental.pallas import tpu as pltpu
from jax.sharding import PartitionSpec as P

MESH = pl.DeviceIdType.MESH
CW = 256
ROW_PARTS = ((0, 96), (96, 80), (176, 80))
ALL = slice(None)
GATHER_STEPS = (
    (("x", (0, 0, 0), (0, 0, 1)), ("y", (0, 0, ALL), (0, 1, ALL)), ("z", (0, ALL, ALL), (1, ALL, ALL))),
    (("y", (0, 0, 0), (0, 1, 0)), ("z", (0, ALL, 0), (1, ALL, 0)), ("x", (ALL, ALL, 0), (ALL, ALL, 1))),
    (("z", (0, 0, 0), (1, 0, 0)), ("x", (ALL, 0, 0), (ALL, 0, 1)), ("y", (ALL, 0, ALL), (ALL, 1, ALL))),
)
SCATTER_STEPS = tuple(tuple((link, dst, src) for link, src, dst in steps[::-1]) for steps in GATHER_STEPS)
LANDING = ((1, 0, ALL, ALL), (1, 1, 0, ALL), (1, 1, 1, 0))


def moe_kernel(ids_ref, gates_ref, x_hbm, w1_hbm, w3_hbm, w2_hbm, out_ref,
               g_buf, acc, sel, dense, hid, w13, w2, pair, x_exp, part, x_res, gate_col,
               routes, gate_recv, pieces, place, slot_row, slot_col, rank_row, rank_col, pack_gate,
               step_send, step_recv, core_send, core_recv, x_sem, w13_sem, w2_sem, res_sem, route_send, route_recv, ready):
    zb, yb, ex = lax.axis_index("ez"), lax.axis_index("ey"), lax.axis_index("ex")
    xb, cb = ex // 2, ex % 2
    peers = {
        "x": (zb, yb, (1 - xb) * 2 + cb),
        "y": (zb, 1 - yb, ex),
        "z": (1 - zb, yb, ex),
        "core": (zb, yb, xb * 2 + 1 - cb),
    }
    tok = x_hbm.shape[0]
    hidden = x_hbm.shape[1]
    chunks = hidden // CW
    experts, _, ff = w1_hbm.shape
    sources = slot_row.shape[0]
    rows = sel.shape[0]
    cap = rows // sources
    per_expert = rows // experts

    def xor(a, b):
        return a + b - 2 * a * b

    def source_of(rel):
        return (xor(zb, rel // 4 % 2) * 8 + xor(yb, rel // 2 % 2) * 4 + xor(xb, rel % 2) * 2 + xor(cb, rel // 8))

    me = zb * 8 + yb * 4 + ex

    def table_copy(hop):
        src, dst = (((0, 0, 0, 0), (0, 0, 0, 1)), ((0, 0, 0), (0, 0, 1)), ((0, 0), (0, 1)), ((0,), (1,)))[hop]
        return pltpu.make_async_remote_copy(routes.at[src], routes.at[dst], route_send.at[hop], route_recv.at[hop],
                                            device_id=peers[("x", "y", "z", "core")[hop]], device_id_type=MESH)

    def gather_copy(c, part, step):
        r0, n = ROW_PARTS[part]
        link, src, dst = GATHER_STEPS[part][step]
        return pltpu.make_async_remote_copy(
            g_buf.at[(c, 0) + src + (pl.ds(r0, n),)], g_buf.at[(c, 0) + dst + (pl.ds(r0, n),)],
            step_send.at[c, part, step], step_recv.at[c, part, step], device_id=peers[link], device_id_type=MESH)

    def gather_core(c):
        return pltpu.make_async_remote_copy(g_buf.at[c, 0], g_buf.at[c, 1], core_send.at[c], core_recv.at[c],
                                            device_id=peers["core"], device_id_type=MESH)

    def scatter_core(k):
        return pltpu.make_async_remote_copy(dense.at[k % 2, 1], g_buf.at[k, 0], core_send.at[k], core_recv.at[k],
                                            device_id=peers["core"], device_id_type=MESH)

    def scatter_copy(k, part, step):
        r0, n = ROW_PARTS[part]
        link, src, _ = SCATTER_STEPS[part][step]
        return pltpu.make_async_remote_copy(
            g_buf.at[(k, 0) + src + (pl.ds(r0, n),)], g_buf.at[(k,) + LANDING[step] + (pl.ds(r0, n),)],
            step_send.at[k, part, step], step_recv.at[k, part, step], device_id=peers[link], device_id_type=MESH)

    def x_copy(c):
        cols = pl.ds(pl.multiple_of(c * CW, CW), CW)
        return pltpu.make_async_copy(x_hbm.at[:, cols], g_buf.at[c, 0, 0, 0, 0], x_sem.at[c])

    def w13_copies(c, e):
        b = e % 2
        k_rows = pl.ds(pl.multiple_of(c * CW, CW), CW)
        return (pltpu.make_async_copy(w1_hbm.at[e, k_rows], w13.at[b, 0], w13_sem.at[b, 0]),
                pltpu.make_async_copy(w3_hbm.at[e, k_rows], w13.at[b, 1], w13_sem.at[b, 1]))

    def w2_copy(k, e):
        cols = pl.ds(pl.multiple_of(k * CW, CW), CW)
        return pltpu.make_async_copy(w2_hbm.at[e, :, cols], w2.at[e], w2_sem.at[e])

    def each(parts, fn):
        for part in parts:
            fn(part)

    PARTS = range(len(ROW_PARTS))

    barrier = pltpu.get_barrier_semaphore()
    for peer in peers.values():
        pl.semaphore_signal(barrier, inc=1, device_id=peer, device_id_type=MESH)
    for c in range(chunks):
        x_copy(c).start()
    res_copy = pltpu.make_async_copy(x_hbm, x_res, res_sem)
    res_copy.start()
    for e in range(2):
        for copy in w13_copies(0, e):
            copy.start()
    for e in range(experts):
        w2_copy(0, e).start()
    top_k = ids_ref.shape[0]
    routes[0, 0, 0, 0, 0:top_k, :] = ids_ref[...].astype(jnp.float32)
    routes[0, 0, 0, 0, top_k:2 * top_k, :] = gates_ref[...]
    part[...] = jnp.zeros(part.shape, part.dtype)
    pl.semaphore_wait(barrier, len(peers))

    @jax.named_scope("start_first")
    def start_first(c):
        x_copy(c).wait()
        each(PARTS, lambda p: gather_copy(c, p, 0).start())

    @jax.named_scope("advance")
    def advance(c, step):
        def one(p):
            gather_copy(c, p, step - 1).wait_recv()
            gather_copy(c, p, step).start()
        each(PARTS, one)

    @jax.named_scope("to_core")
    def to_core(c):
        each(PARTS, lambda p: gather_copy(c, p, 2).wait_recv())
        gather_core(c).start()

    @jax.named_scope("pack")
    def pack(c):
        @pl.loop(0, sources // 8)
        def _(q):
            for u in range(8):
                rel = q * 8 + u
                s = source_of(rel)
                block = g_buf[c, rel // 8, rel // 4 % 2, rel // 2 % 2, rel % 2]
                packed = jnp.dot(place[s], block, preferred_element_type=jnp.float32)
                pair[0, pl.ds(pl.multiple_of(s * cap, cap), cap), :] = packed.astype(jnp.bfloat16)

    def pick(e):
        x_exp[e % 2] = jnp.dot(sel[e * per_expert:(e + 1) * per_expert, :], pair[0], preferred_element_type=jnp.float32).astype(jnp.bfloat16)

    @jax.named_scope("up_project")
    def up_project(c, e):
        for copy in w13_copies(c, e):
            copy.wait()
        erows = slice(e * per_expert, (e + 1) * per_expert)

        def products():
            for j in range(2):
                for n in range(0, ff, CW):
                    acc[j, erows, n:n + CW] += jnp.dot(x_exp[e % 2], w13[e % 2, j, :, n:n + CW], preferred_element_type=jnp.float32)

        if e + 1 < experts:
            products()
            pick(e + 1)
        else:
            @pl.loop(0, (c + chunks) // chunks)
            def _(_):
                products()
        nc, ne = (c, e + 2) if e + 2 < experts else (c + 1, e + 2 - experts)

        @pl.when(nc < chunks)
        def _():
            for copy in w13_copies(nc, ne):
                copy.start()

    def ones_where(mask):
        return jnp.where(mask, 1.0, 0.0).astype(jnp.bfloat16)

    @jax.named_scope("build_tables")
    def build_tables():
        i32, f32, bf16 = jnp.int32, jnp.float32, jnp.bfloat16

        def prefix(n):
            return ones_where(lax.broadcasted_iota(i32, (n, n), 0) <= lax.broadcasted_iota(i32, (n, n), 1))

        for rel in range(sources):
            route = routes.at[rel // 8, rel // 4 % 2, rel // 2 % 2, rel % 2]
            expert = (lax.broadcasted_iota(i32, (experts, tok), 0) + me * experts).astype(f32)
            total = jnp.zeros((experts, tok), f32)
            for j in range(top_k):
                total = total + jnp.where(route[j:j + 1, :] == expert, route[top_k + j:top_k + j + 1, :], 0.0)
            gate_recv[source_of(rel)] = total
        best = gate_recv[:, 0, :]
        for e in range(1, experts):
            best = jnp.maximum(best, gate_recv[:, e, :])
        hit = best > 0.0
        count = jnp.dot(ones_where(hit), prefix(tok), preferred_element_type=f32)
        slots = jnp.where(hit, count - 1.0, -1.0)
        slot_row[...] = slots.astype(i32)
        slots_t = jnp.transpose(jnp.concatenate([slots, jnp.zeros((128 - sources, tok), f32)], axis=0)).astype(i32)
        for s in range(sources):
            slot_col[s * tok:(s + 1) * tok, :] = slots_t[:, s:s + 1]
        for s in range(sources):
            gs = gate_recv[s]
            hi = gs.astype(bf16).astype(f32)
            mid = (gs - hi).astype(bf16).astype(f32)
            pieces[s, 0:experts, :] = jnp.where(gs > 0.0, 1.0, 0.0)
            pieces[s, experts:2 * experts, :] = hi
            pieces[s, 2 * experts:3 * experts, :] = mid
            pieces[s, 3 * experts:4 * experts, :] = gs - hi - mid
        for s in range(sources):
            place[s] = ones_where(slot_row[s:s + 1, :] == lax.broadcasted_iota(i32, (cap, tok), 0))
            packed = lax.dot_general(pieces[s].astype(bf16), place[s], (((1,), (1,)), ((), ())), preferred_element_type=f32)
            rank_row[s * experts:(s + 1) * experts, :] = packed[0:experts].astype(i32)
            pack_gate[s * experts:(s + 1) * experts, :] = packed[experts:2 * experts] + packed[2 * experts:3 * experts] + packed[3 * experts:]
        n = sources * experts
        chosen = rank_row[...].astype(f32)
        count = jnp.dot(chosen.astype(bf16), prefix(cap), preferred_element_type=f32)
        r, c = lax.broadcasted_iota(i32, (n, n), 0), lax.broadcasted_iota(i32, (n, n), 1)
        earlier = ones_where(((r & (experts - 1)) == (c & (experts - 1))) & (c < r))
        before = jnp.sum(jnp.dot(earlier, chosen.astype(bf16), preferred_element_type=f32), axis=1, keepdims=True)
        rank = jnp.where(chosen > 0.0, count + before - 1.0, -1.0)
        rank_row[...] = rank.astype(i32)
        rank_t = jnp.transpose(jnp.concatenate([rank, jnp.zeros((128 - n, cap), f32)], axis=0)).astype(i32)
        for s in range(sources):
            rank_col[s * cap:(s + 1) * cap, :] = rank_t[:, s * experts:(s + 1) * experts]

    @jax.named_scope("build_pick")
    def build_pick(half):
        tile = 128

        @pl.loop(half * rows // tile // 2, (half + 1) * rows // tile // 2)
        def _(t):
            e = t * tile // per_expert
            iota = lax.broadcasted_iota(jnp.int32, (tile, cap), 0) + t * tile % per_expert
            trows = pl.ds(pl.multiple_of(t * tile, tile), tile)
            gate = jnp.zeros((tile, cap), jnp.float32)
            for s in range(sources):
                mask = rank_row[pl.ds(s * experts + e, 1), :] == iota
                sel[trows, s * cap:(s + 1) * cap] = ones_where(mask)
                gate = gate + jnp.where(mask, pack_gate[pl.ds(s * experts + e, 1), :], 0.0)
            gate_col[trows, :] = jnp.sum(gate, axis=1, keepdims=True)

    @jax.named_scope("clear_sums")
    def clear_sums():
        @pl.loop(0, rows // 64)
        def _(t):
            trows = pl.ds(pl.multiple_of(t * 64, 64), 64)
            for j in range(2):
                acc[j, trows, :] = jnp.zeros((64, ff), jnp.float32)

    def table_next(hop):
        table_copy(hop - 1).wait_recv()
        table_copy(hop).start()

    table_copy(0).start()
    start_first(0)
    start_first(1)
    clear_sums()
    table_next(1)
    advance(0, 1)
    start_first(2)
    table_next(2)
    advance(0, 2)
    advance(1, 1)
    table_next(3)
    start_first(3)
    table_copy(3).wait_recv()
    build_tables()
    build_pick(0)
    to_core(0)
    build_pick(1)
    advance(1, 2)
    advance(2, 1)

    @pl.loop(1, chunks + 1)
    def _(k):
        @pl.when(k + 3 < chunks)
        def _():
            start_first(k + 3)

        @pl.when(k + 2 < chunks)
        def _():
            advance(k + 2, 1)

        @pl.when(k + 1 < chunks)
        def _():
            advance(k + 1, 2)

        gather_core(k - 1).wait_recv()
        pack(k - 1)
        @pl.loop(0, (k - 1 + chunks) // chunks)
        def _(_):
            pick(0)

        for e in range(experts // 2):
            up_project(k - 1, e)

        @pl.when(k < chunks)
        def _():
            to_core(k)

        for e in range(experts // 2, experts):
            up_project(k - 1, e)

    @pl.loop(0, chunks)
    def _(c):
        for p in PARTS:
            for step in range(3):
                gather_copy(c, p, step).wait_send()
        gather_core(c).wait_send()

    for hop in range(4):
        table_copy(hop).wait_send()
    for peer in peers.values():
        pl.semaphore_signal(ready, inc=1, device_id=peer, device_id_type=MESH)

    @pl.loop(0, rows // 64)
    def _(t):
        trows = pl.ds(pl.multiple_of(t * 64, 64), 64)
        hid[trows, :] = (jax.nn.silu(acc[0, trows, :]) * acc[1, trows, :]).astype(jnp.bfloat16)
        iota = lax.broadcasted_iota(jnp.int32, (64, per_expert), 1)
        for e in range(experts):
            mask = rank_col[trows, e:e + 1] == iota
            sel[trows, e * per_expert:(e + 1) * per_expert] = jnp.where(mask, 1.0, 0.0).astype(jnp.bfloat16)

    res_copy.wait()
    pl.semaphore_wait(ready, len(peers))

    def add_into(dst, others):
        total = dst[...].astype(jnp.float32)
        for other in others:
            total = total + other[...].astype(jnp.float32)
        dst[...] = total.astype(jnp.bfloat16)

    @jax.named_scope("sum_core")
    def sum_core(k):
        scatter_core(k).wait_recv()

        @pl.loop(0, 8)
        def _(j):
            idx = (j // 4, j // 2 % 2, j % 2)
            add_into(g_buf.at[(k, 0) + idx], [dense.at[(k % 2, 0) + idx]])

    @jax.named_scope("sum_first")
    def sum_first(k):
        for p in PARTS:
            scatter_copy(k, p, 0).wait_recv()
            r0, n = ROW_PARTS[p]
            add_into(g_buf.at[(k, 0) + SCATTER_STEPS[p][0][2] + (pl.ds(r0, n),)], [g_buf.at[(k,) + LANDING[0] + (pl.ds(r0, n),)]])

    @jax.named_scope("sum_second")
    def sum_second(k):
        for p in PARTS:
            scatter_copy(k, p, 1).wait_recv()
            r0, n = ROW_PARTS[p]
            add_into(g_buf.at[(k, 0) + SCATTER_STEPS[p][2][1] + (pl.ds(r0, n),)], [g_buf.at[k, 1, 1, 0, 1, pl.ds(r0, n)]])

    @jax.named_scope("finish")
    def finish(k):
        for p in PARTS:
            scatter_copy(k, p, 2).wait_recv()
        cols = pl.ds(pl.multiple_of(k * CW, CW), CW)
        moe = g_buf[k, 0, 0, 0, 0].astype(jnp.float32) + g_buf[k, 1, 1, 0, 0].astype(jnp.float32) + g_buf[k, 1, 1, 1, 0].astype(jnp.float32)
        out_ref[:, cols] = (x_res[:, cols].astype(jnp.float32) + moe).astype(jnp.bfloat16)

    def start_scatter(k):
        each(PARTS, lambda p: scatter_copy(k, p, 0).start())

    def reduce_step(k):
        @pl.when((k >= 1) & (k <= chunks))
        def _():
            sum_core(k - 1)

        @pl.when((k >= 1) & (k <= chunks))
        def _():
            start_scatter(k - 1)

        @pl.when((k >= 2) & (k <= chunks + 1))
        def _():
            sum_first(k - 2)
            each(PARTS, lambda p: scatter_copy(k - 2, p, 1).start())

        @pl.when((k >= 3) & (k <= chunks + 2))
        def _():
            sum_second(k - 3)
            each(PARTS, lambda p: scatter_copy(k - 3, p, 2).start())

        @pl.when(k >= 4)
        def _():
            finish(k - 4)

    @jax.named_scope("down_project")
    def down_project(k):
        @pl.loop(0, experts // 2)
        def _(half):
            both = (half * 2, half * 2 + 1)
            for e in both:
                w2_copy(k, e).wait()
            for u, e in enumerate(both):
                erows = pl.ds(pl.multiple_of(e * per_expert, per_expert), per_expert)
                o = jnp.dot(hid[erows, :], w2[e], preferred_element_type=jnp.float32) * gate_col[erows, :]
                hi = o.astype(jnp.bfloat16)
                pair[0, erows, :] = hi
                pair[1, erows, :] = (o - hi.astype(jnp.float32)).astype(jnp.bfloat16)

            @pl.when(k + 1 < chunks)
            def _():
                for e in both:
                    w2_copy(k + 1, e).start()

    def combine(k):
        def spread(m):
            for core in range(2):
                s = m * 2 + core
                slots = slot_col[pl.ds(pl.multiple_of(s * tok, tok), tok), :] if not isinstance(s, int) else slot_col[s * tok:(s + 1) * tok, :]
                spot = jnp.where(slots == lax.broadcasted_iota(jnp.int32, (tok, cap), 1), 1.0, 0.0).astype(jnp.bfloat16)
                block = jnp.dot(spot, part[m % 2, core * cap:(core + 1) * cap, :], preferred_element_type=jnp.float32)
                dense[k % 2, xor(core, cb), xor(m // 4, zb), xor(m // 2 % 2, yb), xor(m % 2, xb)] = block.astype(jnp.bfloat16)

        chips = sources // 2

        def half(h):
            @pl.loop(h * chips // 2, (h + 1) * chips // 2)
            def _(m):
                spread((m + chips - 1) % chips)
                chosen = sel[pl.ds(pl.multiple_of(m * 2 * cap, 2 * cap), 2 * cap), :]
                total = jnp.dot(chosen, pair[0], preferred_element_type=jnp.float32)
                total = total + jnp.dot(chosen, pair[1], preferred_element_type=jnp.float32)
                part[m % 2] = total.astype(jnp.bfloat16)

        half(0)
        reduce_step(k)
        half(1)
        spread(chips - 1)

    @pl.loop(0, chunks)
    def _(k):
        down_project(k)

        @pl.when(k >= 2)
        def _():
            scatter_core(k - 2).wait_send()

        combine(k)
        scatter_core(k).start()

    @pl.loop(chunks, chunks + 4)
    def _(k):
        reduce_step(k)

    for k in (chunks - 2, chunks - 1):
        scatter_core(k).wait_send()

    @pl.loop(0, chunks)
    def _(k):
        for p in PARTS:
            for step in range(3):
                scatter_copy(k, p, step).wait_send()


def moe_call(expert_ids, gate_weights, tokens, w_gate, w_up, w_down, devices):
    tok, hidden = tokens.shape
    experts, _, ff = w_gate.shape
    cap = tok * expert_ids.shape[0] // devices
    rows = devices * cap
    chunks = hidden // CW
    bf16, f32, i32 = jnp.bfloat16, jnp.float32, jnp.int32
    vmem = pl.BlockSpec(memory_space=pltpu.VMEM)
    hbm = pl.BlockSpec(memory_space=pl.ANY)
    dma = pltpu.SemaphoreType.DMA
    return pl.pallas_call(
        moe_kernel,
        out_shape=jax.ShapeDtypeStruct((tok, hidden), bf16),
        in_specs=[vmem, vmem, hbm, hbm, hbm, hbm],
        out_specs=vmem,
        scratch_shapes=[
            pltpu.VMEM((chunks, 2, 2, 2, 2, tok, CW), bf16),
            pltpu.VMEM((2, rows, ff), f32),
            pltpu.VMEM((rows, rows), bf16),
            pltpu.VMEM((2, 2, 2, 2, 2, tok, CW), bf16),
            pltpu.VMEM((rows, ff), bf16),
            pltpu.VMEM((2, 2, CW, ff), bf16),
            pltpu.VMEM((experts, ff, CW), bf16),
            pltpu.VMEM((2, rows, CW), bf16),
            pltpu.VMEM((2, rows // experts, CW), bf16),
            pltpu.VMEM((2, 2 * cap, CW), bf16),
            pltpu.VMEM((tok, hidden), bf16),
            pltpu.VMEM((rows, 1), f32),
            pltpu.VMEM((2, 2, 2, 2, 2 * expert_ids.shape[0], tok), f32),
            pltpu.VMEM((devices, experts, tok), f32),
            pltpu.VMEM((devices, 4 * experts, tok), f32),
            pltpu.VMEM((devices, cap, tok), bf16),
            pltpu.VMEM((devices, tok), i32),
            pltpu.VMEM((devices * tok, 1), i32),
            pltpu.VMEM((devices * experts, cap), i32),
            pltpu.VMEM((rows, experts), i32),
            pltpu.VMEM((devices * experts, cap), f32),
            dma((chunks, 3, 3)), dma((chunks, 3, 3)), dma((chunks,)), dma((chunks,)), dma((chunks,)),
            dma((2, 2)), dma((experts,)), dma, dma((4,)), dma((4,)), pltpu.SemaphoreType.REGULAR,
        ],
        compiler_params=pltpu.CompilerParams(collective_id=0, has_side_effects=True, vmem_limit_bytes=67043328),
    )(expert_ids, gate_weights, tokens, w_gate, w_up, w_down)


def solution(mesh):
    ep_axes = tuple(mesh.axis_names)
    num_devices = math.prod(mesh.shape[axis_name] for axis_name in ep_axes)
    row_spec = P(ep_axes, None)
    w_spec = P(ep_axes, None, None)

    def local_layer(tokens, expert_ids, gate_weights, w_gate, w_up, w_down):
        return moe_call(expert_ids.T, gate_weights.T, tokens, w_gate, w_up, w_down, num_devices)

    return jax.shard_map(local_layer, mesh=mesh, in_specs=(row_spec, row_spec, row_spec, w_spec, w_spec, w_spec), out_specs=row_spec, check_vma=False)
```

```python
import math
import jax
import jax.numpy as jnp
from jax import lax
from jax.experimental import pallas as pl
from jax.experimental.pallas import tpu as pltpu
from jax.sharding import PartitionSpec as P

MESH = pl.DeviceIdType.MESH
CW = 256
ROW_PARTS = ((0, 96), (96, 80), (176, 80))
ALL = slice(None)
GATHER_STEPS = (
    (("x", (0, 0, 0), (0, 0, 1)), ("y", (0, 0, ALL), (0, 1, ALL)), ("z", (0, ALL, ALL), (1, ALL, ALL))),
    (("y", (0, 0, 0), (0, 1, 0)), ("z", (0, ALL, 0), (1, ALL, 0)), ("x", (ALL, ALL, 0), (ALL, ALL, 1))),
    (("z", (0, 0, 0), (1, 0, 0)), ("x", (ALL, 0, 0), (ALL, 0, 1)), ("y", (ALL, 0, ALL), (ALL, 1, ALL))),
)
SCATTER_STEPS = tuple(tuple((link, dst, src) for link, src, dst in steps[::-1]) for steps in GATHER_STEPS)
LANDING = ((1, 0, ALL, ALL), (1, 1, 0, ALL), (1, 1, 1, 0))


def moe_kernel(ids_ref, gates_ref, x_hbm, w1_hbm, w3_hbm, w2_hbm, out_ref,
               g_buf, acc, sel, dense, hid, w13, w2, pair, x_exp, part, x_res, gate_col,
               routes, gate_recv, pieces, place, slot_row, slot_col, rank_row, rank_col, pack_gate,
               step_send, step_recv, core_send, core_recv, x_sem, w13_sem, w2_sem, res_sem, route_send, route_recv, ready):
    zb, yb, ex = lax.axis_index("ez"), lax.axis_index("ey"), lax.axis_index("ex")
    xb, cb = ex // 2, ex % 2
    peers = {
        "x": (zb, yb, (1 - xb) * 2 + cb),
        "y": (zb, 1 - yb, ex),
        "z": (1 - zb, yb, ex),
        "core": (zb, yb, xb * 2 + 1 - cb),
    }
    tok = x_hbm.shape[0]
    hidden = x_hbm.shape[1]
    chunks = hidden // CW
    experts, _, ff = w1_hbm.shape
    sources = slot_row.shape[0]
    rows = sel.shape[0]
    cap = rows // sources
    per_expert = rows // experts

    def xor(a, b):
        return a + b - 2 * a * b

    def source_of(rel):
        return (xor(zb, rel // 4 % 2) * 8 + xor(yb, rel // 2 % 2) * 4 + xor(xb, rel % 2) * 2 + xor(cb, rel // 8))

    me = zb * 8 + yb * 4 + ex

    def table_copy(hop):
        src, dst = (((0, 0, 0, 0), (0, 0, 0, 1)), ((0, 0, 0), (0, 0, 1)), ((0, 0), (0, 1)), ((0,), (1,)))[hop]
        return pltpu.make_async_remote_copy(routes.at[src], routes.at[dst], route_send.at[hop], route_recv.at[hop],
                                            device_id=peers[("x", "y", "z", "core")[hop]], device_id_type=MESH)

    def gather_copy(c, part, step):
        r0, n = ROW_PARTS[part]
        link, src, dst = GATHER_STEPS[part][step]
        return pltpu.make_async_remote_copy(
            g_buf.at[(c, 0) + src + (pl.ds(r0, n),)], g_buf.at[(c, 0) + dst + (pl.ds(r0, n),)],
            step_send.at[c, part, step], step_recv.at[c, part, step], device_id=peers[link], device_id_type=MESH)

    def gather_core(c):
        return pltpu.make_async_remote_copy(g_buf.at[c, 0], g_buf.at[c, 1], core_send.at[c], core_recv.at[c],
                                            device_id=peers["core"], device_id_type=MESH)

    def scatter_core(k):
        return pltpu.make_async_remote_copy(dense.at[k % 2, 1], g_buf.at[k, 0], core_send.at[k], core_recv.at[k],
                                            device_id=peers["core"], device_id_type=MESH)

    def scatter_copy(k, part, step):
        r0, n = ROW_PARTS[part]
        link, src, _ = SCATTER_STEPS[part][step]
        return pltpu.make_async_remote_copy(
            g_buf.at[(k, 0) + src + (pl.ds(r0, n),)], g_buf.at[(k,) + LANDING[step] + (pl.ds(r0, n),)],
            step_send.at[k, part, step], step_recv.at[k, part, step], device_id=peers[link], device_id_type=MESH)

    def x_copy(c):
        cols = pl.ds(pl.multiple_of(c * CW, CW), CW)
        return pltpu.make_async_copy(x_hbm.at[:, cols], g_buf.at[c, 0, 0, 0, 0], x_sem.at[c])

    def w13_copies(c, e):
        b = e % 2
        k_rows = pl.ds(pl.multiple_of(c * CW, CW), CW)
        return (pltpu.make_async_copy(w1_hbm.at[e, k_rows], w13.at[b, 0], w13_sem.at[b, 0]),
                pltpu.make_async_copy(w3_hbm.at[e, k_rows], w13.at[b, 1], w13_sem.at[b, 1]))

    def w2_copy(k, e):
        cols = pl.ds(pl.multiple_of(k * CW, CW), CW)
        return pltpu.make_async_copy(w2_hbm.at[e, :, cols], w2.at[e], w2_sem.at[e])

    def each(parts, fn):
        for part in parts:
            fn(part)

    PARTS = range(len(ROW_PARTS))

    barrier = pltpu.get_barrier_semaphore()
    for peer in peers.values():
        pl.semaphore_signal(barrier, inc=1, device_id=peer, device_id_type=MESH)
    for c in range(chunks):
        x_copy(c).start()
    res_copy = pltpu.make_async_copy(x_hbm, x_res, res_sem)
    res_copy.start()
    for e in range(2):
        for copy in w13_copies(0, e):
            copy.start()
    for e in range(experts):
        w2_copy(0, e).start()
    top_k = ids_ref.shape[0]
    routes[0, 0, 0, 0, 0:top_k, :] = ids_ref[...].astype(jnp.float32)
    routes[0, 0, 0, 0, top_k:2 * top_k, :] = gates_ref[...]
    part[...] = jnp.zeros(part.shape, part.dtype)
    pl.semaphore_wait(barrier, len(peers))

    @jax.named_scope("start_first")
    def start_first(c):
        x_copy(c).wait()
        each(PARTS, lambda p: gather_copy(c, p, 0).start())

    @jax.named_scope("advance")
    def advance(c, step):
        def one(p):
            gather_copy(c, p, step - 1).wait_recv()
            gather_copy(c, p, step).start()
        each(PARTS, one)

    @jax.named_scope("to_core")
    def to_core(c):
        each(PARTS, lambda p: gather_copy(c, p, 2).wait_recv())
        gather_core(c).start()

    @jax.named_scope("pack")
    def pack(c):
        @pl.loop(0, sources // 8)
        def _(q):
            for u in range(8):
                rel = q * 8 + u
                s = source_of(rel)
                block = g_buf[c, rel // 8, rel // 4 % 2, rel // 2 % 2, rel % 2]
                packed = jnp.dot(place[s], block, preferred_element_type=jnp.float32)
                pair[0, pl.ds(pl.multiple_of(s * cap, cap), cap), :] = packed.astype(jnp.bfloat16)

    def pick(e):
        x_exp[e % 2] = jnp.dot(sel[e * per_expert:(e + 1) * per_expert, :], pair[0], preferred_element_type=jnp.float32).astype(jnp.bfloat16)

    @jax.named_scope("up_project")
    def up_project(c, e):
        for copy in w13_copies(c, e):
            copy.wait()
        erows = slice(e * per_expert, (e + 1) * per_expert)

        def products():
            for j in range(2):
                for n in range(0, ff, CW):
                    acc[j, erows, n:n + CW] += jnp.dot(x_exp[e % 2], w13[e % 2, j, :, n:n + CW], preferred_element_type=jnp.float32)

        if e + 1 < experts:
            products()
            pick(e + 1)
        else:
            @pl.loop(0, (c + chunks) // chunks)
            def _(_):
                products()
        nc, ne = (c, e + 2) if e + 2 < experts else (c + 1, e + 2 - experts)

        @pl.when(nc < chunks)
        def _():
            for copy in w13_copies(nc, ne):
                copy.start()

    def ones_where(mask):
        return jnp.where(mask, 1.0, 0.0).astype(jnp.bfloat16)

    @jax.named_scope("build_tables")
    def build_tables():
        i32, f32, bf16 = jnp.int32, jnp.float32, jnp.bfloat16

        def prefix(n):
            return ones_where(lax.broadcasted_iota(i32, (n, n), 0) <= lax.broadcasted_iota(i32, (n, n), 1))

        for rel in range(sources):
            route = routes.at[rel // 8, rel // 4 % 2, rel // 2 % 2, rel % 2]
            expert = (lax.broadcasted_iota(i32, (experts, tok), 0) + me * experts).astype(f32)
            total = jnp.zeros((experts, tok), f32)
            for j in range(top_k):
                total = total + jnp.where(route[j:j + 1, :] == expert, route[top_k + j:top_k + j + 1, :], 0.0)
            gate_recv[source_of(rel)] = total
        best = gate_recv[:, 0, :]
        for e in range(1, experts):
            best = jnp.maximum(best, gate_recv[:, e, :])
        hit = best > 0.0
        count = jnp.dot(ones_where(hit), prefix(tok), preferred_element_type=f32)
        slots = jnp.where(hit, count - 1.0, -1.0)
        slot_row[...] = slots.astype(i32)
        slots_t = jnp.transpose(jnp.concatenate([slots, jnp.zeros((128 - sources, tok), f32)], axis=0)).astype(i32)
        for s in range(sources):
            slot_col[s * tok:(s + 1) * tok, :] = slots_t[:, s:s + 1]
        for s in range(sources):
            gs = gate_recv[s]
            hi = gs.astype(bf16).astype(f32)
            mid = (gs - hi).astype(bf16).astype(f32)
            pieces[s, 0:experts, :] = jnp.where(gs > 0.0, 1.0, 0.0)
            pieces[s, experts:2 * experts, :] = hi
            pieces[s, 2 * experts:3 * experts, :] = mid
            pieces[s, 3 * experts:4 * experts, :] = gs - hi - mid
        for s in range(sources):
            place[s] = ones_where(slot_row[s:s + 1, :] == lax.broadcasted_iota(i32, (cap, tok), 0))
            packed = lax.dot_general(pieces[s].astype(bf16), place[s], (((1,), (1,)), ((), ())), preferred_element_type=f32)
            rank_row[s * experts:(s + 1) * experts, :] = packed[0:experts].astype(i32)
            pack_gate[s * experts:(s + 1) * experts, :] = packed[experts:2 * experts] + packed[2 * experts:3 * experts] + packed[3 * experts:]
        n = sources * experts
        chosen = rank_row[...].astype(f32)
        count = jnp.dot(chosen.astype(bf16), prefix(cap), preferred_element_type=f32)
        r, c = lax.broadcasted_iota(i32, (n, n), 0), lax.broadcasted_iota(i32, (n, n), 1)
        earlier = ones_where(((r & (experts - 1)) == (c & (experts - 1))) & (c < r))
        before = jnp.sum(jnp.dot(earlier, chosen.astype(bf16), preferred_element_type=f32), axis=1, keepdims=True)
        rank = jnp.where(chosen > 0.0, count + before - 1.0, -1.0)
        rank_row[...] = rank.astype(i32)
        rank_t = jnp.transpose(jnp.concatenate([rank, jnp.zeros((128 - n, cap), f32)], axis=0)).astype(i32)
        for s in range(sources):
            rank_col[s * cap:(s + 1) * cap, :] = rank_t[:, s * experts:(s + 1) * experts]

    @jax.named_scope("build_pick")
    def build_pick(half):
        tile = 128

        @pl.loop(half * rows // tile // 2, (half + 1) * rows // tile // 2)
        def _(t):
            e = t * tile // per_expert
            iota = lax.broadcasted_iota(jnp.int32, (tile, cap), 0) + t * tile % per_expert
            trows = pl.ds(pl.multiple_of(t * tile, tile), tile)
            gate = jnp.zeros((tile, cap), jnp.float32)
            for s in range(sources):
                mask = rank_row[pl.ds(s * experts + e, 1), :] == iota
                sel[trows, s * cap:(s + 1) * cap] = ones_where(mask)
                gate = gate + jnp.where(mask, pack_gate[pl.ds(s * experts + e, 1), :], 0.0)
            gate_col[trows, :] = jnp.sum(gate, axis=1, keepdims=True)

    @jax.named_scope("clear_sums")
    def clear_sums():
        @pl.loop(0, rows // 64)
        def _(t):
            trows = pl.ds(pl.multiple_of(t * 64, 64), 64)
            for j in range(2):
                acc[j, trows, :] = jnp.zeros((64, ff), jnp.float32)

    def table_next(hop):
        table_copy(hop - 1).wait_recv()
        table_copy(hop).start()

    table_copy(0).start()
    start_first(0)
    start_first(1)
    clear_sums()
    table_next(1)
    advance(0, 1)
    start_first(2)
    table_next(2)
    advance(0, 2)
    advance(1, 1)
    table_next(3)
    start_first(3)
    advance(2, 1)
    table_copy(3).wait_recv()
    build_tables()
    build_pick(0)
    to_core(0)
    build_pick(1)
    advance(1, 2)

    @pl.loop(1, chunks + 1)
    def _(k):
        @pl.when(k + 3 < chunks)
        def _():
            start_first(k + 3)

        @pl.when(k + 2 < chunks)
        def _():
            advance(k + 2, 1)

        gather_core(k - 1).wait_recv()
        pack(k - 1)
        @pl.loop(0, (k - 1 + chunks) // chunks)
        def _(_):
            pick(0)

        for e in range(experts // 2):
            up_project(k - 1, e)

        @pl.when(k + 1 < chunks)
        def _():
            advance(k + 1, 2)

        @pl.when(k < chunks)
        def _():
            to_core(k)

        for e in range(experts // 2, experts):
            up_project(k - 1, e)

    @pl.loop(0, chunks)
    def _(c):
        for p in PARTS:
            for step in range(3):
                gather_copy(c, p, step).wait_send()
        gather_core(c).wait_send()

    for hop in range(4):
        table_copy(hop).wait_send()
    for peer in peers.values():
        pl.semaphore_signal(ready, inc=1, device_id=peer, device_id_type=MESH)

    @pl.loop(0, rows // 64)
    def _(t):
        trows = pl.ds(pl.multiple_of(t * 64, 64), 64)
        hid[trows, :] = (jax.nn.silu(acc[0, trows, :]) * acc[1, trows, :]).astype(jnp.bfloat16)
        iota = lax.broadcasted_iota(jnp.int32, (64, per_expert), 1)
        for e in range(experts):
            mask = rank_col[trows, e:e + 1] == iota
            sel[trows, e * per_expert:(e + 1) * per_expert] = jnp.where(mask, 1.0, 0.0).astype(jnp.bfloat16)

    res_copy.wait()
    pl.semaphore_wait(ready, len(peers))

    def add_into(dst, others):
        total = dst[...].astype(jnp.float32)
        for other in others:
            total = total + other[...].astype(jnp.float32)
        dst[...] = total.astype(jnp.bfloat16)

    @jax.named_scope("sum_core")
    def sum_core(k):
        scatter_core(k).wait_recv()

        @pl.loop(0, 8)
        def _(j):
            idx = (j // 4, j // 2 % 2, j % 2)
            add_into(g_buf.at[(k, 0) + idx], [dense.at[(k % 2, 0) + idx]])

    @jax.named_scope("sum_first")
    def sum_first(k):
        for p in PARTS:
            scatter_copy(k, p, 0).wait_recv()
            r0, n = ROW_PARTS[p]
            add_into(g_buf.at[(k, 0) + SCATTER_STEPS[p][0][2] + (pl.ds(r0, n),)], [g_buf.at[(k,) + LANDING[0] + (pl.ds(r0, n),)]])

    @jax.named_scope("sum_second")
    def sum_second(k):
        for p in PARTS:
            scatter_copy(k, p, 1).wait_recv()
            r0, n = ROW_PARTS[p]
            add_into(g_buf.at[(k, 0) + SCATTER_STEPS[p][2][1] + (pl.ds(r0, n),)], [g_buf.at[k, 1, 1, 0, 1, pl.ds(r0, n)]])

    @jax.named_scope("finish")
    def finish(k):
        for p in PARTS:
            scatter_copy(k, p, 2).wait_recv()
        cols = pl.ds(pl.multiple_of(k * CW, CW), CW)
        moe = g_buf[k, 0, 0, 0, 0].astype(jnp.float32) + g_buf[k, 1, 1, 0, 0].astype(jnp.float32) + g_buf[k, 1, 1, 1, 0].astype(jnp.float32)
        out_ref[:, cols] = (x_res[:, cols].astype(jnp.float32) + moe).astype(jnp.bfloat16)

    def start_scatter(k):
        each(PARTS, lambda p: scatter_copy(k, p, 0).start())

    def reduce_step(k):
        @pl.when((k >= 1) & (k <= chunks))
        def _():
            sum_core(k - 1)

        @pl.when((k >= 1) & (k <= chunks))
        def _():
            start_scatter(k - 1)

        @pl.when((k >= 2) & (k <= chunks + 1))
        def _():
            sum_first(k - 2)
            each(PARTS, lambda p: scatter_copy(k - 2, p, 1).start())

        @pl.when((k >= 3) & (k <= chunks + 2))
        def _():
            sum_second(k - 3)
            each(PARTS, lambda p: scatter_copy(k - 3, p, 2).start())

        @pl.when(k >= 4)
        def _():
            finish(k - 4)

    @jax.named_scope("down_project")
    def down_project(k):
        @pl.loop(0, experts // 2)
        def _(half):
            both = (half * 2, half * 2 + 1)
            for e in both:
                w2_copy(k, e).wait()
            for u, e in enumerate(both):
                erows = pl.ds(pl.multiple_of(e * per_expert, per_expert), per_expert)
                o = jnp.dot(hid[erows, :], w2[e], preferred_element_type=jnp.float32) * gate_col[erows, :]
                hi = o.astype(jnp.bfloat16)
                pair[0, erows, :] = hi
                pair[1, erows, :] = (o - hi.astype(jnp.float32)).astype(jnp.bfloat16)

            @pl.when(k + 1 < chunks)
            def _():
                for e in both:
                    w2_copy(k + 1, e).start()

    def combine(k):
        def spread(m):
            for core in range(2):
                s = m * 2 + core
                slots = slot_col[pl.ds(pl.multiple_of(s * tok, tok), tok), :] if not isinstance(s, int) else slot_col[s * tok:(s + 1) * tok, :]
                spot = jnp.where(slots == lax.broadcasted_iota(jnp.int32, (tok, cap), 1), 1.0, 0.0).astype(jnp.bfloat16)
                block = jnp.dot(spot, part[m % 2, core * cap:(core + 1) * cap, :], preferred_element_type=jnp.float32)
                dense[k % 2, xor(core, cb), xor(m // 4, zb), xor(m // 2 % 2, yb), xor(m % 2, xb)] = block.astype(jnp.bfloat16)

        chips = sources // 2

        def half(h):
            @pl.loop(h * chips // 2, (h + 1) * chips // 2)
            def _(m):
                spread((m + chips - 1) % chips)
                chosen = sel[pl.ds(pl.multiple_of(m * 2 * cap, 2 * cap), 2 * cap), :]
                total = jnp.dot(chosen, pair[0], preferred_element_type=jnp.float32)
                total = total + jnp.dot(chosen, pair[1], preferred_element_type=jnp.float32)
                part[m % 2] = total.astype(jnp.bfloat16)

        half(0)
        reduce_step(k)
        half(1)
        spread(chips - 1)

    @pl.loop(0, chunks)
    def _(k):
        down_project(k)

        @pl.when(k >= 2)
        def _():
            scatter_core(k - 2).wait_send()

        combine(k)
        scatter_core(k).start()

    @pl.loop(chunks, chunks + 4)
    def _(k):
        reduce_step(k)

    for k in (chunks - 2, chunks - 1):
        scatter_core(k).wait_send()

    @pl.loop(0, chunks)
    def _(k):
        for p in PARTS:
            for step in range(3):
                scatter_copy(k, p, step).wait_send()


def moe_call(expert_ids, gate_weights, tokens, w_gate, w_up, w_down, devices):
    tok, hidden = tokens.shape
    experts, _, ff = w_gate.shape
    cap = tok * expert_ids.shape[0] // devices
    rows = devices * cap
    chunks = hidden // CW
    bf16, f32, i32 = jnp.bfloat16, jnp.float32, jnp.int32
    vmem = pl.BlockSpec(memory_space=pltpu.VMEM)
    hbm = pl.BlockSpec(memory_space=pl.ANY)
    dma = pltpu.SemaphoreType.DMA
    return pl.pallas_call(
        moe_kernel,
        out_shape=jax.ShapeDtypeStruct((tok, hidden), bf16),
        in_specs=[vmem, vmem, hbm, hbm, hbm, hbm],
        out_specs=vmem,
        scratch_shapes=[
            pltpu.VMEM((chunks, 2, 2, 2, 2, tok, CW), bf16),
            pltpu.VMEM((2, rows, ff), f32),
            pltpu.VMEM((rows, rows), bf16),
            pltpu.VMEM((2, 2, 2, 2, 2, tok, CW), bf16),
            pltpu.VMEM((rows, ff), bf16),
            pltpu.VMEM((2, 2, CW, ff), bf16),
            pltpu.VMEM((experts, ff, CW), bf16),
            pltpu.VMEM((2, rows, CW), bf16),
            pltpu.VMEM((2, rows // experts, CW), bf16),
            pltpu.VMEM((2, 2 * cap, CW), bf16),
            pltpu.VMEM((tok, hidden), bf16),
            pltpu.VMEM((rows, 1), f32),
            pltpu.VMEM((2, 2, 2, 2, 2 * expert_ids.shape[0], tok), f32),
            pltpu.VMEM((devices, experts, tok), f32),
            pltpu.VMEM((devices, 4 * experts, tok), f32),
            pltpu.VMEM((devices, cap, tok), bf16),
            pltpu.VMEM((devices, tok), i32),
            pltpu.VMEM((devices * tok, 1), i32),
            pltpu.VMEM((devices * experts, cap), i32),
            pltpu.VMEM((rows, experts), i32),
            pltpu.VMEM((devices * experts, cap), f32),
            dma((chunks, 3, 3)), dma((chunks, 3, 3)), dma((chunks,)), dma((chunks,)), dma((chunks,)),
            dma((2, 2)), dma((experts,)), dma, dma((4,)), dma((4,)), pltpu.SemaphoreType.REGULAR,
        ],
        compiler_params=pltpu.CompilerParams(collective_id=0, has_side_effects=True, vmem_limit_bytes=67043328),
    )(expert_ids, gate_weights, tokens, w_gate, w_up, w_down)


def solution(mesh):
    ep_axes = tuple(mesh.axis_names)
    num_devices = math.prod(mesh.shape[axis_name] for axis_name in ep_axes)
    row_spec = P(ep_axes, None)
    w_spec = P(ep_axes, None, None)

    def local_layer(tokens, expert_ids, gate_weights, w_gate, w_up, w_down):
        return moe_call(expert_ids.T, gate_weights.T, tokens, w_gate, w_up, w_down, num_devices)

    return jax.shard_map(local_layer, mesh=mesh, in_specs=(row_spec, row_spec, row_spec, w_spec, w_spec, w_spec), out_specs=row_spec, check_vma=False)
```
